32 devices in a mesh: dp: 2 (over x), tp: 4 (over z), pp: 4 (over y, core).
Axes of the slice: x: 2, y: 2, z: 4, core: 2. Of those that a mesh axis runs over, the one named last changes fastest.
Arguments:
- hidden_in: bfloat16 [512, 2560], P('dp'), parts along dimension 0
- positions: int32 [512], P('dp'), parts along dimension 0
- k_cache: bfloat16 [4, 512, 32, 8, 128], P('pp', 'dp', None, 'tp'), parts along dimension 1
- v_cache: bfloat16 [4, 512, 32, 8, 128], P('pp', 'dp', None, 'tp'), parts along dimension 1
- attn_gain: bfloat16 [4, 2560], P('pp')
- w_q: bfloat16 [4, 2560, 4096], P('pp', None, 'tp')
- w_k: bfloat16 [4, 2560, 1024], P('pp', None, 'tp')
- w_v: bfloat16 [4, 2560, 1024], P('pp', None, 'tp')
- w_o: bfloat16 [4, 4096, 2560], P('pp', 'tp')
- mlp_gain: bfloat16 [4, 2560], P('pp')
- w_gate: bfloat16 [4, 2560, 9728], P('pp', None, 'tp')
- w_up: bfloat16 [4, 2560, 9728], P('pp', None, 'tp')
- w_down: bfloat16 [4, 9728, 2560], P('pp', 'tp')
- final_gain: bfloat16 [2560], replicated
Outputs:
- output 1: bfloat16 [512, 2560], P('dp'), parts along dimension 0
- output 2: bfloat16 [4, 512, 8, 128], P('pp', 'dp', 'tp'), parts along dimension 1
- output 3: bfloat16 [4, 512, 8, 128], P('pp', 'dp', 'tp'), parts along dimension 1
There are 2 independent parts. The reference program is written for one: setup_inputs(seed, part) draws one part's arguments, and reference() takes and returns one part's arrays. A program takes and returns all parts, laid end to end along the dimension named above; an argument that names none is the same for every part.
All inputs are finite; a program needn't handle non-finite values.
Results may differ from the reference program's by a relative error of at most 0.02.
Values are sent between devices in bfloat16 or wider.
A program may use at most 1 GiB of HBM per device.

```python
import jax
import jax.numpy as jnp
from jax import lax

D = 2560
HEADS = 32
KV_HEADS = 8
HEAD_DIM = 128
FF = 9728
LAYERS = 4
BATCH = 256
CACHE_LEN = 32

RMS_EPS = 1e-5
ROPE_THETA = 500000.0
GROUP_SIZE = HEADS // KV_HEADS
POS_LOW = CACHE_LEN // 8


def setup_inputs(seed: int = 0, part: int = 0) -> dict:
    base_key = jax.random.key(seed)
    part_key = jax.random.fold_in(base_key, part)
    weight_keys = jax.random.split(base_key, 11)
    part_keys = jax.random.split(part_key, 5)
    q_width = HEADS * HEAD_DIM
    kv_width = KV_HEADS * HEAD_DIM
    in_scale = D ** -0.5
    out_scale = (CACHE_LEN / 8) ** 0.5 * q_width ** -0.5

    def normal_bf(rng_key, arr_shape, std_scale):
        return (jax.random.normal(rng_key, arr_shape, jnp.float32) * std_scale).astype(jnp.bfloat16)

    def gain_bf(rng_key, arr_shape):
        return jax.random.uniform(rng_key, arr_shape, jnp.float32, 0.5, 1.5).astype(jnp.bfloat16)

    pos_draw = jax.random.randint(part_keys[1], (BATCH,), POS_LOW, CACHE_LEN, jnp.int32)
    shuffle_idx = jax.random.permutation(part_keys[2], BATCH)
    pos_draw = pos_draw.at[shuffle_idx[0]].set(CACHE_LEN - 1).at[shuffle_idx[1]].set(POS_LOW)
    cache_shape = (LAYERS, BATCH, CACHE_LEN, KV_HEADS, HEAD_DIM)
    return {
        'hidden_in': normal_bf(part_keys[0], (BATCH, D), 1.0),
        'positions': pos_draw,
        'k_cache': normal_bf(part_keys[3], cache_shape, 1.0),
        'v_cache': normal_bf(part_keys[4], cache_shape, 1.0),
        'attn_gain': gain_bf(weight_keys[0], (LAYERS, D)),
        'w_q': normal_bf(weight_keys[1], (LAYERS, D, q_width), in_scale),
        'w_k': normal_bf(weight_keys[2], (LAYERS, D, kv_width), in_scale),
        'w_v': normal_bf(weight_keys[3], (LAYERS, D, kv_width), in_scale),
        'w_o': normal_bf(weight_keys[4], (LAYERS, q_width, D), out_scale),
        'mlp_gain': gain_bf(weight_keys[5], (LAYERS, D)),
        'w_gate': normal_bf(weight_keys[6], (LAYERS, D, FF), in_scale),
        'w_up': normal_bf(weight_keys[7], (LAYERS, D, FF), in_scale),
        'w_down': normal_bf(weight_keys[8], (LAYERS, FF, D), FF ** -0.5),
        'final_gain': jax.random.uniform(weight_keys[9], (D,), jnp.float32, 0.1, 1.9).astype(jnp.bfloat16),
    }


def rms_norm(hidden, gain_vec):
    hidden32 = hidden.astype(jnp.float32)
    mean_sq = jnp.mean(hidden32 * hidden32, axis=-1, keepdims=True)
    return (hidden32 * lax.rsqrt(mean_sq + RMS_EPS) * gain_vec.astype(jnp.float32)).astype(jnp.bfloat16)


def rope_tables(positions):
    freq_idx = jnp.arange(0, HEAD_DIM, 2).astype(jnp.float32)
    inv_freq = ROPE_THETA ** (-freq_idx / HEAD_DIM)
    angles = positions.astype(jnp.float32)[:, None] * inv_freq[None, :]
    return jnp.cos(angles), jnp.sin(angles)


def apply_rope(head_vals, cos_t, sin_t):
    half_dim = head_vals.shape[-1] // 2
    heads32 = head_vals.astype(jnp.float32)
    first_half = heads32[..., :half_dim]
    second_half = heads32[..., half_dim:]
    cos_b = cos_t[:, None, :]
    sin_b = sin_t[:, None, :]
    return jnp.concatenate([first_half * cos_b - second_half * sin_b, second_half * cos_b + first_half * sin_b], axis=-1).astype(jnp.bfloat16)


def reference(hidden_in, positions, k_cache, v_cache, attn_gain, w_q, w_k, w_v, w_o, mlp_gain, w_gate, w_up, w_down, final_gain):
    cos_t, sin_t = rope_tables(positions)
    cache_mask = jnp.arange(CACHE_LEN)[None, :] < positions[:, None]
    score_scale = HEAD_DIM ** -0.5

    def layer_step(hidden, layer_args):
        gain_attn, q_weight, k_weight, v_weight, o_weight, gain_mlp, gate_weight, up_weight, down_weight, k_layer, v_layer = layer_args
        normed = rms_norm(hidden, gain_attn)
        queries = jnp.dot(normed, q_weight, preferred_element_type=jnp.float32).astype(jnp.bfloat16)
        queries = apply_rope(queries.reshape(BATCH, HEADS, HEAD_DIM), cos_t, sin_t)
        queries = queries.reshape(BATCH, KV_HEADS, GROUP_SIZE, HEAD_DIM).astype(jnp.float32)
        keys_new = jnp.dot(normed, k_weight, preferred_element_type=jnp.float32).astype(jnp.bfloat16)
        keys_new = apply_rope(keys_new.reshape(BATCH, KV_HEADS, HEAD_DIM), cos_t, sin_t)
        vals_new = jnp.dot(normed, v_weight, preferred_element_type=jnp.float32).astype(jnp.bfloat16).reshape(BATCH, KV_HEADS, HEAD_DIM)
        scores = jnp.einsum('bgrh,btgh->bgrt', queries, k_layer.astype(jnp.float32)) * score_scale
        score_new = jnp.einsum('bgrh,bgh->bgr', queries, keys_new.astype(jnp.float32)) * score_scale
        scores = jnp.where(cache_mask[:, None, None, :], scores, -jnp.inf)
        top_score = jnp.maximum(jnp.max(scores, axis=-1), score_new)
        exp_scores = jnp.exp(scores - top_score[..., None])
        exp_new = jnp.exp(score_new - top_score)
        denominator = jnp.sum(exp_scores, axis=-1) + exp_new
        prob_cache = (exp_scores / denominator[..., None]).astype(jnp.bfloat16).astype(jnp.float32)
        prob_new = (exp_new / denominator).astype(jnp.bfloat16).astype(jnp.float32)
        context = jnp.einsum('bgrt,btgh->bgrh', prob_cache, v_layer.astype(jnp.float32))
        context = context + prob_new[..., None] * vals_new.astype(jnp.float32)[:, :, None, :]
        context = context.astype(jnp.bfloat16).reshape(BATCH, HEADS * HEAD_DIM)
        attn_out = jnp.dot(context, o_weight, preferred_element_type=jnp.float32).astype(jnp.bfloat16)
        hidden = (hidden.astype(jnp.float32) + attn_out.astype(jnp.float32)).astype(jnp.bfloat16)
        mlp_in = rms_norm(hidden, gain_mlp)
        gate_val = jnp.dot(mlp_in, gate_weight, preferred_element_type=jnp.float32).astype(jnp.bfloat16)
        up_val = jnp.dot(mlp_in, up_weight, preferred_element_type=jnp.float32).astype(jnp.bfloat16)
        act_val = (jax.nn.silu(gate_val.astype(jnp.float32)) * up_val.astype(jnp.float32)).astype(jnp.bfloat16)
        mlp_out = jnp.dot(act_val, down_weight, preferred_element_type=jnp.float32).astype(jnp.bfloat16)
        hidden = (hidden.astype(jnp.float32) + mlp_out.astype(jnp.float32)).astype(jnp.bfloat16)
        return hidden, (keys_new, vals_new)

    hidden, new_rows = lax.scan(layer_step, hidden_in, (attn_gain, w_q, w_k, w_v, w_o, mlp_gain, w_gate, w_up, w_down, k_cache, v_cache))
    return rms_norm(hidden, final_gain), new_rows[0], new_rows[1]
```

```python
import functools

import jax
import jax.numpy as jnp
from jax import lax
from jax.experimental import pallas as pl
from jax.experimental.pallas import tpu as pltpu
from jax.sharding import PartitionSpec as P

RMS_EPS = 1e-5
ROPE_THETA = 500000.0
BF16 = jnp.bfloat16
F32 = jnp.float32
MESH = pl.DeviceIdType.MESH

N_CHUNK = 4
N_SUB = 5
GROUP = 16


def rope_tables(positions, head_dim):
    freq_idx = jnp.arange(0, head_dim, 2).astype(F32)
    inv_freq = ROPE_THETA ** (-freq_idx / head_dim)
    angles = positions.astype(F32)[:, None] * inv_freq[None, :]
    return jnp.cos(angles), jnp.sin(angles)


def norm_rows(rows, gain):
    rows32 = rows.astype(F32)
    mean_sq = jnp.mean(rows32 * rows32, axis=-1, keepdims=True)
    return (rows32 * lax.rsqrt(mean_sq + RMS_EPS) * gain.astype(F32)).astype(BF16)


def dot(a, b):
    return jnp.dot(a, b, preferred_element_type=F32)


def column_blocks(width, size):
    return [(at, min(size, width - at)) for at in range(0, width, size)]


def step_kernel(
    n_stage, n_tp,
    hid, pos, cos_t, sin_t, k_hbm, v_hbm, gain_a, w_q, w_k, w_v, w_o, gain_m, w_g, w_u, w_d, gain_f,
    out, k_out, v_out,
    wq, wk, wv, wg, wu, wd, kb, vb, hb, nb, qb, kn, vn, cb, ab, slots,
    part, rec_e, rec_m, res_a, res_b, hrec0, hrec1, hrec_m, hres,
    s_w, s_kv, s_rows, s_out, s_fwd,
    r_h, s_h, r_out, s_part, s_sum, s_res, r_e, r_m, r_a, r_b,
    s_hsum, s_hres0, s_hres1, r_h0, r_h1, r_hm,
):
    rows = hb.shape[1]
    sub = part.shape[3]
    half = N_SUB * sub
    d_attn = cb.shape[1]
    kv_width = kn.shape[2]
    head_dim = kb.shape[2]
    n_head = d_attn // head_dim
    kv_heads = kv_width // head_dim
    per_kv = n_head // kv_heads
    cache_len = kb.shape[1] // (rows * kv_heads)
    stage = lax.axis_index('pp')
    line = lax.axis_index('tp')
    side = stage // 2
    helped = lax.rem(stage + 2, n_stage)
    is_mid = jnp.logical_or(line == 1, line == n_tp - 2)
    is_end = jnp.logical_not(is_mid)
    mid_of = jnp.where(line < n_tp // 2, 1, n_tp - 2)
    end_of = jnp.where(line < n_tp // 2, 0, n_tp - 1)
    other_mid = n_tp - 1 - line

    def remote(src, dst, send, recv, to_stage, to_line):
        return pltpu.make_async_remote_copy(
            src_ref=src, dst_ref=dst, send_sem=send, recv_sem=recv,
            device_id={'pp': to_stage, 'tp': to_line}, device_id_type=MESH)

    def landed(ref, sem):
        pltpu.make_async_copy(ref, ref, sem).wait()

    barrier = pltpu.get_barrier_semaphore()
    for other_stage in range(n_stage):
        for other_line in range(n_tp):
            pl.semaphore_signal(barrier, inc=1, device_id={'pp': other_stage, 'tp': other_line}, device_id_type=MESH)

    @pl.when(stage == 0)
    def _():
        for c in range(N_CHUNK):
            pltpu.make_async_copy(hid.at[c], hb.at[c], r_h.at[c]).start()

    def load_kv(c, slot):
        return (pltpu.make_async_copy(k_hbm.at[c], kb.at[slot], s_kv.at[0, slot]),
                pltpu.make_async_copy(v_hbm.at[c], vb.at[slot], s_kv.at[1, slot]))

    o_rows = w_o.shape[0]
    loads = [
        pltpu.make_async_copy(w_q, wq, s_w.at[0]),
        pltpu.make_async_copy(w_k, wk, s_w.at[1]),
        pltpu.make_async_copy(w_v, wv, s_w.at[2]),
        pltpu.make_async_copy(w_o, wd.at[pl.ds(0, o_rows)], s_w.at[3]),
        pltpu.make_async_copy(w_g, wg, s_w.at[4]),
        pltpu.make_async_copy(w_u, wu, s_w.at[5]),
        pltpu.make_async_copy(w_d.at[pl.ds(o_rows, w_d.shape[0] - o_rows)], wd.at[pl.ds(o_rows, w_d.shape[0] - o_rows)], s_w.at[6]),
        pltpu.make_async_copy(w_d.at[pl.ds(0, o_rows)], wd.at[pl.ds(0, o_rows)], s_w.at[7]),
    ]
    for one in loads[:3]:
        one.start()
    for one in load_kv(0, 0):
        one.start()
    loads[3].start()

    @pl.when(stage > 0)
    def _():
        for one in loads[4:7]:
            one.start()
        pl.semaphore_wait(barrier, n_stage * n_tp)

    row_id = lax.broadcasted_iota(jnp.int32, slots.shape, 0)
    col_id = lax.broadcasted_iota(jnp.int32, slots.shape, 1)
    keys_per_row = cache_len * kv_heads
    quad = slots.shape[1] // keys_per_row
    same_row = lax.rem(row_id, quad) == col_id // keys_per_row
    same_head = lax.rem(col_id, kv_heads) == row_id // (GROUP * per_kv)
    slots[...] = jnp.where(jnp.logical_and(same_row, same_head), lax.rem(col_id, keys_per_row) // kv_heads, cache_len)

    def send_part(k, b_half):
        kc = lax.rem(k, N_CHUNK)
        base = N_SUB if b_half else 0
        if b_half:
            @pl.when(is_end)
            def _():
                for s in range(N_SUB):
                    remote(part.at[kc, base + s], hrec0.at[kc, s], s_part.at[kc, base + s], r_h0.at[kc, s], helped, mid_of).start()

            @pl.when(is_mid)
            def _():
                for s in range(N_SUB):
                    remote(part.at[kc, base + s], hrec1.at[kc, s], s_part.at[kc, base + s], r_h1.at[kc, s], helped, line).start()
        else:
            @pl.when(is_end)
            def _():
                for s in range(N_SUB):
                    remote(part.at[kc, s], rec_e.at[kc, s], s_part.at[kc, s], r_e.at[kc, s], stage, mid_of).start()

    def wait_part_sends(k):
        kc = lax.rem(k, N_CHUNK)
        for s in range(N_SUB):
            landed(part.at[kc, N_SUB + s], s_part.at[kc, N_SUB + s])

        @pl.when(is_end)
        def _():
            for s in range(N_SUB):
                landed(part.at[kc, s], s_part.at[kc, s])

        @pl.when(is_mid)
        def _():
            for s in range(N_SUB):
                landed(part.at[kc, s], s_sum.at[kc, s])

    def sum_first(k):
        kc = lax.rem(k, N_CHUNK)
        for s in range(N_SUB):
            landed(rec_e.at[kc, s], r_e.at[kc, s])
            part[kc, s] = part[kc, s] + rec_e[kc, s]
            remote(part.at[kc, s], rec_m.at[k, s], s_sum.at[kc, s], r_m.at[k, s], stage, other_mid).start()

    def sum_second(k):
        kc = lax.rem(k, N_CHUNK)

        @pl.when(k >= N_CHUNK)
        def _():
            for s in range(N_SUB):
                landed(res_a.at[kc, s], s_res.at[kc, s])

        for s in range(N_SUB):
            landed(rec_m.at[k, s], r_m.at[k, s])
            res_a[kc, s] = (part[kc, s] + rec_m[k, s]).astype(BF16)
            remote(res_a.at[kc, s], res_a.at[kc, s], s_res.at[kc, s], r_a.at[kc, s], stage, end_of).start()

    def help_first(k):
        kc = lax.rem(k, N_CHUNK)
        for s in range(N_SUB):
            landed(hrec0.at[kc, s], r_h0.at[kc, s])
            landed(hrec1.at[kc, s], r_h1.at[kc, s])
            hrec1[kc, s] = hrec1[kc, s] + hrec0[kc, s]
            remote(hrec1.at[kc, s], hrec_m.at[k, s], s_hsum.at[kc, s], r_hm.at[k, s], stage, other_mid).start()

    def help_second(k):
        kc = lax.rem(k, N_CHUNK)

        @pl.when(k >= N_CHUNK)
        def _():
            for s in range(N_SUB):
                landed(hres.at[kc, s], s_hres0.at[kc, s])
                landed(hres.at[kc, s], s_hres1.at[kc, s])

        for s in range(N_SUB):
            landed(hrec_m.at[k, s], r_hm.at[k, s])
            landed(hrec1.at[kc, s], s_hsum.at[kc, s])
            hres[kc, s] = (hrec1[kc, s] + hrec_m[k, s]).astype(BF16)
            remote(hres.at[kc, s], res_b.at[kc, s], s_hres0.at[kc, s], r_b.at[kc, s], helped, end_of).start()
            remote(hres.at[kc, s], res_b.at[kc, s], s_hres1.at[kc, s], r_b.at[kc, s], helped, line).start()

    def help_stage():
        @pl.when(is_mid)
        def _():
            @pl.loop(0, 2 * N_CHUNK + 1)
            def _(k):
                @pl.when(k < 2 * N_CHUNK)
                def _():
                    help_first(k)

                @pl.when(k >= 1)
                def _():
                    help_second(k - 1)

    def relay(k):
        @pl.when(is_mid)
        def _():
            @pl.when(jnp.logical_and(k >= 1, k <= 2 * N_CHUNK))
            def _():
                sum_first(k - 1)

            @pl.when(jnp.logical_and(k >= 2, k <= 2 * N_CHUNK + 1))
            def _():
                sum_second(k - 2)

    def add_sum(c):
        @pl.when(is_end)
        def _():
            for s in range(N_SUB):
                landed(res_a.at[c, s], r_a.at[c, s])

        for s in range(N_SUB):
            at = pl.ds(s * sub, sub)
            hb[c, :, at] = (hb[c, :, at].astype(F32) + res_a[c, s].astype(F32)).astype(BF16)
        for s in range(N_SUB):
            at = pl.ds(half + s * sub, sub)
            landed(res_b.at[c, s], r_b.at[c, s])
            hb[c, :, at] = (hb[c, :, at].astype(F32) + res_b[c, s].astype(F32)).astype(BF16)

    def partials(k, act, weight, depth):
        kc = lax.rem(k, N_CHUNK)
        for b_half in (True, False):
            base = N_SUB if b_half else 0
            got = dot(act, weight[pl.ds(0, depth), pl.ds(half if b_half else 0, half)])
            for s in range(N_SUB):
                part[kc, base + s] = got[:, s * sub:(s + 1) * sub]
            send_part(k, b_half)

    def attention(c):
        slot = lax.rem(c, 2)
        landed(hb.at[c], r_h.at[c])

        @pl.when(c == 0)
        def _():
            for one in loads[:3]:
                one.wait()

        normed = norm_rows(hb[c], gain_a[...])
        base = pl.multiple_of(c * rows, rows)
        cosv = cos_t[pl.ds(base, rows), :]
        sinv = sin_t[pl.ds(base, rows), :]

        def rope(vals):
            vals32 = vals.astype(BF16).astype(F32)
            return (vals32 * cosv + pltpu.roll(vals32, head_dim // 2, 1) * sinv).astype(BF16)

        nb[...] = normed
        got_k = dot(nb[...], wk[...])
        got_v = dot(nb[...], wv[...])
        for g in range(kv_heads):
            at = pl.ds(g * head_dim, head_dim)
            kn[c, :, at] = rope(got_k[:, g * head_dim:(g + 1) * head_dim])
        vn[c] = got_v.astype(BF16)
        pltpu.make_async_copy(kn.at[c], k_out.at[c], s_rows.at[0, c]).start()
        pltpu.make_async_copy(vn.at[c], v_out.at[c], s_rows.at[1, c]).start()
        got_q = dot(nb[...], wq[...])
        for h in range(n_head):
            qb[:, pl.ds(h * head_dim, head_dim)] = rope(got_q[:, h * head_dim:(h + 1) * head_dim])

        for one in load_kv(c, slot):
            one.wait()
        scale = head_dim ** -0.5
        keys = slots.shape[1]
        n_quad = GROUP // quad
        rows_id = lax.broadcasted_iota(jnp.int32, (GROUP * n_head, keys), 0)
        quad_of = lax.rem(rows_id, GROUP) // quad
        slot_of = slots[...]
        groups = range(rows // GROUP)
        queries = []
        scores = []
        for g in groups:
            rows_at = pl.ds(g * GROUP, GROUP)
            queries.append(jnp.concatenate([qb[rows_at, pl.ds(h * head_dim, head_dim)] for h in range(n_head)], axis=0))
            picked = None
            for j in range(n_quad):
                key_block = kb[slot, pl.ds(g * GROUP * keys_per_row + j * keys, keys), :]
                one = lax.dot_general(queries[g], key_block, (((1,), (1,)), ((), ())), preferred_element_type=F32)
                picked = one if picked is None else jnp.where(quad_of == j, one, picked)
            scores.append(picked * scale)
        probs = []
        probs_new = []
        values_new = []
        for g in groups:
            rows_at = pl.ds(g * GROUP, GROUP)
            key_new = jnp.concatenate([kn[c, rows_at, pl.ds((h // per_kv) * head_dim, head_dim)] for h in range(n_head)], axis=0)
            values_new.append(jnp.concatenate([vn[c, rows_at, pl.ds((h // per_kv) * head_dim, head_dim)] for h in range(n_head)], axis=0))
            score_new = jnp.sum(queries[g].astype(F32) * key_new.astype(F32), axis=-1, keepdims=True) * scale
            p_rows = pos[pl.ds(pl.multiple_of(base + g * GROUP, GROUP), GROUP), :]
            p_wide = jnp.concatenate([jnp.concatenate([p_rows] * (keys // p_rows.shape[1]), axis=1)] * n_head, axis=0)
            valid = slot_of < p_wide
            masked = jnp.where(valid, scores[g], -jnp.inf)
            top = jnp.maximum(jnp.max(masked, axis=-1, keepdims=True), score_new)
            exps = jnp.exp(masked - top)
            exp_new = jnp.exp(score_new - top)
            total = jnp.sum(exps, axis=-1, keepdims=True) + exp_new
            probs.append(exps / total)
            probs_new.append((exp_new / total).astype(BF16).astype(F32))
        for g in groups:
            context = None
            for j in range(n_quad):
                val_block = vb[slot, pl.ds(g * GROUP * keys_per_row + j * keys, keys), :]
                one = dot(jnp.where(quad_of == j, probs[g], 0.0).astype(BF16), val_block)
                context = one if context is None else context + one
            context = (context + probs_new[g] * values_new[g].astype(F32)).astype(BF16)
            for h in range(n_head):
                cb[pl.ds(g * GROUP, GROUP), pl.ds(h * head_dim, head_dim)] = context[h * GROUP:(h + 1) * GROUP]

    def attn_part(c):
        @pl.when(c + 1 < N_CHUNK)
        def _():
            for one in load_kv(c + 1, lax.rem(c + 1, 2)):
                one.start()

        attention(c)

        @pl.when(c == 0)
        def _():
            loads[3].wait()

            @pl.when(stage == 0)
            def _():
                for one in loads[4:7]:
                    one.start()
                pl.semaphore_wait(barrier, n_stage * n_tp)

        partials(c, cb[...], wd, o_rows)

        @pl.when(c == N_CHUNK - 1)
        def _():
            loads[7].start()

    def mlp_part(k):
        c = k - N_CHUNK
        add_sum(c)
        nb[...] = norm_rows(hb[c], gain_m[...])

        @pl.when(c == 0)
        def _():
            for one in loads[4:6]:
                one.wait()

        for at, size in column_blocks(wg.shape[1], 512):
            gate = dot(nb[...], wg[:, pl.ds(at, size)]).astype(BF16).astype(F32)
            up = dot(nb[...], wu[:, pl.ds(at, size)]).astype(BF16).astype(F32)
            ab[:, pl.ds(at, size)] = (gate * jax.nn.sigmoid(gate) * up).astype(BF16)

        @pl.when(c == 0)
        def _():
            for one in loads[6:]:
                one.wait()

        wait_part_sends(k - N_CHUNK)
        partials(k, ab[...], wd, wd.shape[0])

    def finish(c):
        add_sum(c)

        @pl.when(stage < n_stage - 1)
        def _():
            remote(hb.at[c], hb.at[c], s_h.at[c], r_h.at[c], stage + 1, line).start()

        @pl.when(stage == n_stage - 1)
        def _():
            hb[c] = norm_rows(hb[c], gain_f[...])
            remote(hb.at[c], out.at[c], s_fwd.at[0, c], r_out.at[c], stage - 2, line).start()
            remote(hb.at[c], out.at[c], s_fwd.at[1, c], r_out.at[c], stage - 1, line).start()
            pltpu.make_async_copy(hb.at[c], out.at[c], s_out.at[c]).start()

    def compute_stage():
        @pl.loop(0, N_CHUNK)
        def _(k):
            attn_part(k)
            relay(k)

        @pl.loop(N_CHUNK, 2 * N_CHUNK)
        def _(k):
            mlp_part(k)
            relay(k)

        @pl.loop(2 * N_CHUNK, 3 * N_CHUNK)
        def _(k):
            finish(k - 2 * N_CHUNK)
            relay(k)

    @pl.when(side == 1)
    def _():
        help_stage()

    compute_stage()

    @pl.when(side == 0)
    def _():
        help_stage()

    @pl.loop(0, N_CHUNK)
    def _(c):
        wait_part_sends(c)
        for i, (ref, dst) in enumerate(((kn, k_out), (vn, v_out))):
            landed(ref.at[c], s_rows.at[i, c])

        @pl.when(is_mid)
        def _():
            for s in range(N_SUB):
                landed(res_a.at[c, s], s_res.at[c, s])
                landed(hres.at[c, s], s_hres0.at[c, s])
                landed(hres.at[c, s], s_hres1.at[c, s])

        @pl.when(stage < n_stage - 1)
        def _():
            landed(hb.at[c], s_h.at[c])
            landed(out.at[c], r_out.at[c])

        @pl.when(stage == n_stage - 3)
        def _():
            remote(out.at[c], out.at[c], s_fwd.at[0, c], r_out.at[c], stage - 1, line).start()

        @pl.when(stage == n_stage - 1)
        def _():
            landed(hb.at[c], s_out.at[c])
            landed(hb.at[c], s_fwd.at[0, c])
            landed(hb.at[c], s_fwd.at[1, c])

    @pl.when(stage == n_stage - 3)
    def _():
        for c in range(N_CHUNK):
            landed(out.at[c], s_fwd.at[0, c])


def solution(mesh):
    n_stage = mesh.shape['pp']
    n_tp = mesh.shape['tp']
    cache_spec = P('pp', 'dp', None, 'tp', None)
    gain_spec = P('pp', None)
    col_spec = P('pp', None, 'tp')
    row_spec = P('pp', 'tp', None)
    rows_spec = P('pp', 'dp', 'tp', None)

    def stage_fn(hidden_in, positions, k_cache, v_cache, attn_gain, w_q, w_k, w_v, w_o, mlp_gain, w_gate, w_up, w_down, final_gain):
        batch, d_model = hidden_in.shape
        _, _, cache_len, kv_local, head_dim = k_cache.shape
        rows = batch // N_CHUNK
        d_attn = w_q.shape[2]
        kv_width = kv_local * head_dim
        d_ff = w_gate.shape[2]
        half = d_model // 2
        sub = half // N_SUB
        n_head = d_attn // head_dim
        keys = rows * cache_len * kv_local
        score_keys = 4 * cache_len * kv_local
        cos_h, sin_h = rope_tables(positions, head_dim)
        cos_t = jnp.concatenate([cos_h, cos_h], axis=-1)
        sin_t = jnp.concatenate([-sin_h, sin_h], axis=-1)
        pos_wide = jnp.broadcast_to(positions[:, None], (batch, 128))
        anywhere = pl.BlockSpec(memory_space=pl.ANY)
        vmem = pl.BlockSpec(memory_space=pltpu.VMEM)
        dma = pltpu.SemaphoreType.DMA
        blocks = (N_CHUNK, N_SUB)
        call = pl.pallas_call(
            functools.partial(step_kernel, n_stage, n_tp),
            out_shape=[
                jax.ShapeDtypeStruct((N_CHUNK, rows, d_model), BF16),
                jax.ShapeDtypeStruct((N_CHUNK, rows, kv_width), BF16),
                jax.ShapeDtypeStruct((N_CHUNK, rows, kv_width), BF16),
            ],
            in_specs=[anywhere, vmem, vmem, vmem, anywhere, anywhere, vmem] + [anywhere] * 4 + [vmem] + [anywhere] * 3 + [vmem],
            out_specs=[anywhere] * 3,
            scratch_shapes=[
                pltpu.VMEM((d_model, d_attn), BF16),
                pltpu.VMEM((d_model, kv_width), BF16),
                pltpu.VMEM((d_model, kv_width), BF16),
                pltpu.VMEM((d_model, d_ff), BF16),
                pltpu.VMEM((d_model, d_ff), BF16),
                pltpu.VMEM((d_ff, d_model), BF16),
                pltpu.VMEM((2, keys, head_dim), BF16),
                pltpu.VMEM((2, keys, head_dim), BF16),
                pltpu.VMEM((N_CHUNK, rows, d_model), BF16),
                pltpu.VMEM((rows, d_model), BF16),
                pltpu.VMEM((rows, d_attn), BF16),
                pltpu.VMEM((N_CHUNK, rows, kv_width), BF16),
                pltpu.VMEM((N_CHUNK, rows, kv_width), BF16),
                pltpu.VMEM((rows, d_attn), BF16),
                pltpu.VMEM((rows, d_ff), BF16),
                pltpu.VMEM((GROUP * n_head, score_keys), jnp.int32),
                pltpu.VMEM((N_CHUNK, 2 * N_SUB, rows, sub), F32),
                pltpu.VMEM(blocks + (rows, sub), F32),
                pltpu.VMEM((2 * N_CHUNK, N_SUB, rows, sub), F32),
                pltpu.VMEM(blocks + (rows, sub), BF16),
                pltpu.VMEM(blocks + (rows, sub), BF16),
                pltpu.VMEM(blocks + (rows, sub), F32),
                pltpu.VMEM(blocks + (rows, sub), F32),
                pltpu.VMEM((2 * N_CHUNK, N_SUB, rows, sub), F32),
                pltpu.VMEM(blocks + (rows, sub), BF16),
                dma((8,)), dma((2, 2)), dma((2, N_CHUNK)), dma((N_CHUNK,)), dma((2, N_CHUNK)),
                dma((N_CHUNK,)), dma((N_CHUNK,)), dma((N_CHUNK,)),
                dma((N_CHUNK, 2 * N_SUB)), dma(blocks), dma(blocks),
                dma(blocks), dma((2 * N_CHUNK, N_SUB)), dma(blocks), dma(blocks),
                dma(blocks), dma(blocks), dma(blocks), dma(blocks), dma(blocks), dma((2 * N_CHUNK, N_SUB)),
            ],
            compiler_params=pltpu.CompilerParams(collective_id=0, has_side_effects=True, vmem_limit_bytes=67043328),
        )
        out, k_rows, v_rows = call(
            hidden_in.reshape(N_CHUNK, rows, d_model), pos_wide, cos_t, sin_t,
            k_cache.reshape(N_CHUNK, keys, head_dim), v_cache.reshape(N_CHUNK, keys, head_dim),
            attn_gain, w_q[0], w_k[0], w_v[0], w_o[0], mlp_gain, w_gate[0], w_up[0], w_down[0], final_gain[None])
        shape = (1, batch, kv_local, head_dim)
        return out.reshape(batch, d_model), k_rows.reshape(shape), v_rows.reshape(shape)

    return jax.shard_map(
        stage_fn,
        mesh=mesh,
        in_specs=(P('dp', None), P('dp'), cache_spec, cache_spec, gain_spec, col_spec, col_spec, col_spec, row_spec, gain_spec, col_spec, col_spec, row_spec, P(None)),
        out_specs=(P('dp', None), rows_spec, rows_spec),
        check_vma=False,
    )
```

```python
import functools

import jax
import jax.numpy as jnp
from jax import lax
from jax.experimental import pallas as pl
from jax.experimental.pallas import tpu as pltpu
from jax.sharding import PartitionSpec as P

RMS_EPS = 1e-5
ROPE_THETA = 500000.0
BF16 = jnp.bfloat16
F32 = jnp.float32
MESH = pl.DeviceIdType.MESH

N_CHUNK = 4
N_SUB = 5
GROUP = 16


def rope_tables(positions, head_dim):
    freq_idx = jnp.arange(0, head_dim, 2).astype(F32)
    inv_freq = ROPE_THETA ** (-freq_idx / head_dim)
    angles = positions.astype(F32)[:, None] * inv_freq[None, :]
    return jnp.cos(angles), jnp.sin(angles)


def norm_rows(rows, gain):
    rows32 = rows.astype(F32)
    mean_sq = jnp.mean(rows32 * rows32, axis=-1, keepdims=True)
    return (rows32 * lax.rsqrt(mean_sq + RMS_EPS) * gain.astype(F32)).astype(BF16)


def dot(a, b):
    return jnp.dot(a, b, preferred_element_type=F32)


def column_blocks(width, size):
    return [(at, min(size, width - at)) for at in range(0, width, size)]


def step_kernel(
    n_stage, n_tp,
    hid, pos, cos_t, sin_t, k_hbm, v_hbm, gain_a, w_q, w_k, w_v, w_o, gain_m, w_g, w_u, w_d, gain_f,
    out, k_out, v_out,
    wq, wk, wv, wg, wu, wd, kb, vb, hb, nb, qb, kn, vn, cb, ab, slots,
    part, rec_e, rec_m, res_a, res_b, hrec0, hrec1, hrec_m, hres,
    s_w, s_kv, s_rows, s_out, s_fwd,
    r_h, s_h, r_out, s_part, s_sum, s_res, r_e, r_m, r_a, r_b,
    s_hsum, s_hres0, s_hres1, r_h0, r_h1, r_hm,
):
    rows = hb.shape[1]
    sub = part.shape[3]
    half = N_SUB * sub
    d_attn = cb.shape[1]
    kv_width = kn.shape[2]
    head_dim = kb.shape[2]
    n_head = d_attn // head_dim
    kv_heads = kv_width // head_dim
    per_kv = n_head // kv_heads
    cache_len = kb.shape[1] // (rows * kv_heads)
    stage = lax.axis_index('pp')
    line = lax.axis_index('tp')
    side = stage // 2
    helped = lax.rem(stage + 2, n_stage)
    is_mid = jnp.logical_or(line == 1, line == n_tp - 2)
    is_end = jnp.logical_not(is_mid)
    mid_of = jnp.where(line < n_tp // 2, 1, n_tp - 2)
    end_of = jnp.where(line < n_tp // 2, 0, n_tp - 1)
    other_mid = n_tp - 1 - line

    def remote(src, dst, send, recv, to_stage, to_line):
        return pltpu.make_async_remote_copy(
            src_ref=src, dst_ref=dst, send_sem=send, recv_sem=recv,
            device_id={'pp': to_stage, 'tp': to_line}, device_id_type=MESH)

    def landed(ref, sem):
        pltpu.make_async_copy(ref, ref, sem).wait()

    barrier = pltpu.get_barrier_semaphore()
    for other_stage in range(n_stage):
        for other_line in range(n_tp):
            pl.semaphore_signal(barrier, inc=1, device_id={'pp': other_stage, 'tp': other_line}, device_id_type=MESH)

    @pl.when(stage == 0)
    def _():
        for c in range(N_CHUNK):
            pltpu.make_async_copy(hid.at[c], hb.at[c], r_h.at[c]).start()

    def load_kv(c, slot):
        return (pltpu.make_async_copy(k_hbm.at[c], kb.at[slot], s_kv.at[0, slot]),
                pltpu.make_async_copy(v_hbm.at[c], vb.at[slot], s_kv.at[1, slot]))

    o_rows = w_o.shape[0]
    loads = [
        pltpu.make_async_copy(w_q, wq, s_w.at[0]),
        pltpu.make_async_copy(w_k, wk, s_w.at[1]),
        pltpu.make_async_copy(w_v, wv, s_w.at[2]),
        pltpu.make_async_copy(w_o, wd.at[pl.ds(0, o_rows)], s_w.at[3]),
        pltpu.make_async_copy(w_g, wg, s_w.at[4]),
        pltpu.make_async_copy(w_u, wu, s_w.at[5]),
        pltpu.make_async_copy(w_d.at[pl.ds(o_rows, w_d.shape[0] - o_rows)], wd.at[pl.ds(o_rows, w_d.shape[0] - o_rows)], s_w.at[6]),
        pltpu.make_async_copy(w_d.at[pl.ds(0, o_rows)], wd.at[pl.ds(0, o_rows)], s_w.at[7]),
    ]
    for one in loads[:3]:
        one.start()
    for one in load_kv(0, 0):
        one.start()
    loads[3].start()

    @pl.when(stage > 0)
    def _():
        for one in loads[4:7]:
            one.start()
        pl.semaphore_wait(barrier, n_stage * n_tp)

    row_id = lax.broadcasted_iota(jnp.int32, slots.shape, 0)
    col_id = lax.broadcasted_iota(jnp.int32, slots.shape, 1)
    keys_per_row = cache_len * kv_heads
    quad = slots.shape[1] // keys_per_row
    same_row = lax.rem(row_id, quad) == col_id // keys_per_row
    same_head = lax.rem(col_id, kv_heads) == row_id // (GROUP * per_kv)
    slots[...] = jnp.where(jnp.logical_and(same_row, same_head), lax.rem(col_id, keys_per_row) // kv_heads, cache_len)

    def send_part(k, b_half):
        kc = lax.rem(k, N_CHUNK)
        base = N_SUB if b_half else 0
        if b_half:
            @pl.when(is_end)
            def _():
                for s in range(N_SUB):
                    remote(part.at[kc, base + s], hrec_m.at[k, s], s_part.at[kc, base + s], r_hm.at[k, s], helped, line).start()

            @pl.when(is_mid)
            def _():
                for s in range(N_SUB):
                    remote(part.at[kc, base + s], hrec1.at[kc, s], s_part.at[kc, base + s], r_h1.at[kc, s], helped, line).start()
        else:
            @pl.when(is_end)
            def _():
                for s in range(N_SUB):
                    remote(part.at[kc, s], rec_e.at[kc, s], s_part.at[kc, s], r_e.at[kc, s], stage, mid_of).start()

    def wait_part_sends(k):
        kc = lax.rem(k, N_CHUNK)
        for s in range(N_SUB):
            landed(part.at[kc, N_SUB + s], s_part.at[kc, N_SUB + s])

        @pl.when(is_end)
        def _():
            for s in range(N_SUB):
                landed(part.at[kc, s], s_part.at[kc, s])

        @pl.when(is_mid)
        def _():
            for s in range(N_SUB):
                landed(part.at[kc, s], s_sum.at[kc, s])

    def sum_first(k):
        kc = lax.rem(k, N_CHUNK)
        for s in range(N_SUB):
            landed(rec_e.at[kc, s], r_e.at[kc, s])
            part[kc, s] = part[kc, s] + rec_e[kc, s]
            remote(part.at[kc, s], rec_m.at[k, s], s_sum.at[kc, s], r_m.at[k, s], stage, other_mid).start()

    def sum_second(k):
        kc = lax.rem(k, N_CHUNK)

        @pl.when(k >= N_CHUNK)
        def _():
            for s in range(N_SUB):
                landed(res_a.at[kc, s], s_res.at[kc, s])

        for s in range(N_SUB):
            landed(rec_m.at[k, s], r_m.at[k, s])
            res_a[kc, s] = (part[kc, s] + rec_m[k, s]).astype(BF16)
            remote(res_a.at[kc, s], res_a.at[kc, s], s_res.at[kc, s], r_a.at[kc, s], stage, end_of).start()

    def help_first(k):
        kc = lax.rem(k, N_CHUNK)
        for s in range(N_SUB):
            landed(hrec0.at[kc, s], r_h0.at[kc, s])
            landed(hrec1.at[kc, s], r_h1.at[kc, s])
            hrec1[kc, s] = hrec1[kc, s] + hrec0[kc, s]
            remote(hrec1.at[kc, s], hrec_m.at[k, s], s_hsum.at[kc, s], r_hm.at[k, s], stage, other_mid).start()

    def help_second(k):
        kc = lax.rem(k, N_CHUNK)

        @pl.when(k >= N_CHUNK)
        def _():
            for s in range(N_SUB):
                landed(hres.at[kc, s], s_hres0.at[kc, s])
                landed(hres.at[kc, s], s_hres1.at[kc, s])

        for s in range(N_SUB):
            landed(hrec_m.at[k, s], r_hm.at[k, s])
            landed(hrec1.at[kc, s], s_hsum.at[kc, s])
            hres[kc, s] = (hrec1[kc, s] + hrec_m[k, s]).astype(BF16)
            remote(hres.at[kc, s], res_b.at[kc, s], s_hres0.at[kc, s], r_b.at[kc, s], helped, end_of).start()
            remote(hres.at[kc, s], res_b.at[kc, s], s_hres1.at[kc, s], r_b.at[kc, s], helped, line).start()

    def help_forward(k):
        kc = lax.rem(k, N_CHUNK)

        @pl.when(k >= N_CHUNK)
        def _():
            for s in range(N_SUB):
                landed(hrec0.at[kc, s], s_hsum.at[kc, s])

        for s in range(N_SUB):
            landed(hrec_m.at[k, s], r_hm.at[k, s])
            remote(hrec_m.at[k, s], hrec0.at[kc, s], s_hsum.at[kc, s], r_h0.at[kc, s], stage, mid_of).start()

    def help_stage():
        @pl.when(is_end)
        def _():
            @pl.loop(0, 2 * N_CHUNK)
            def _(k):
                help_forward(k)

        @pl.when(is_mid)
        def _():
            @pl.loop(0, 2 * N_CHUNK + 1)
            def _(k):
                @pl.when(k < 2 * N_CHUNK)
                def _():
                    help_first(k)

                @pl.when(k >= 1)
                def _():
                    help_second(k - 1)

    def relay(k):
        @pl.when(is_mid)
        def _():
            @pl.when(jnp.logical_and(k >= 1, k <= 2 * N_CHUNK))
            def _():
                sum_first(k - 1)

            @pl.when(jnp.logical_and(k >= 2, k <= 2 * N_CHUNK + 1))
            def _():
                sum_second(k - 2)

    def add_sum(c):
        @pl.when(is_end)
        def _():
            for s in range(N_SUB):
                landed(res_a.at[c, s], r_a.at[c, s])

        for s in range(N_SUB):
            at = pl.ds(s * sub, sub)
            hb[c, :, at] = (hb[c, :, at].astype(F32) + res_a[c, s].astype(F32)).astype(BF16)
        for s in range(N_SUB):
            at = pl.ds(half + s * sub, sub)
            landed(res_b.at[c, s], r_b.at[c, s])
            hb[c, :, at] = (hb[c, :, at].astype(F32) + res_b[c, s].astype(F32)).astype(BF16)

    def partials(k, act, weight, depth):
        kc = lax.rem(k, N_CHUNK)
        for b_half in (True, False):
            base = N_SUB if b_half else 0
            got = dot(act, weight[pl.ds(0, depth), pl.ds(half if b_half else 0, half)])
            for s in range(N_SUB):
                part[kc, base + s] = got[:, s * sub:(s + 1) * sub]
            send_part(k, b_half)

    def attention(c):
        slot = lax.rem(c, 2)
        landed(hb.at[c], r_h.at[c])

        @pl.when(c == 0)
        def _():
            for one in loads[:3]:
                one.wait()

        normed = norm_rows(hb[c], gain_a[...])
        base = pl.multiple_of(c * rows, rows)
        cosv = cos_t[pl.ds(base, rows), :]
        sinv = sin_t[pl.ds(base, rows), :]

        def rope(vals):
            vals32 = vals.astype(BF16).astype(F32)
            return (vals32 * cosv + pltpu.roll(vals32, head_dim // 2, 1) * sinv).astype(BF16)

        nb[...] = normed
        got_k = dot(nb[...], wk[...])
        got_v = dot(nb[...], wv[...])
        for g in range(kv_heads):
            at = pl.ds(g * head_dim, head_dim)
            kn[c, :, at] = rope(got_k[:, g * head_dim:(g + 1) * head_dim])
        vn[c] = got_v.astype(BF16)
        pltpu.make_async_copy(kn.at[c], k_out.at[c], s_rows.at[0, c]).start()
        pltpu.make_async_copy(vn.at[c], v_out.at[c], s_rows.at[1, c]).start()
        got_q = dot(nb[...], wq[...])
        for h in range(n_head):
            qb[:, pl.ds(h * head_dim, head_dim)] = rope(got_q[:, h * head_dim:(h + 1) * head_dim])

        for one in load_kv(c, slot):
            one.wait()
        scale = head_dim ** -0.5
        keys = slots.shape[1]
        n_quad = GROUP // quad
        rows_id = lax.broadcasted_iota(jnp.int32, (GROUP * n_head, keys), 0)
        quad_of = lax.rem(rows_id, GROUP) // quad
        slot_of = slots[...]
        groups = range(rows // GROUP)
        queries = []
        scores = []
        for g in groups:
            rows_at = pl.ds(g * GROUP, GROUP)
            queries.append(jnp.concatenate([qb[rows_at, pl.ds(h * head_dim, head_dim)] for h in range(n_head)], axis=0))
            picked = None
            for j in range(n_quad):
                key_block = kb[slot, pl.ds(g * GROUP * keys_per_row + j * keys, keys), :]
                one = lax.dot_general(queries[g], key_block, (((1,), (1,)), ((), ())), preferred_element_type=F32)
                picked = one if picked is None else jnp.where(quad_of == j, one, picked)
            scores.append(picked * scale)
        probs = []
        probs_new = []
        values_new = []
        for g in groups:
            rows_at = pl.ds(g * GROUP, GROUP)
            key_new = jnp.concatenate([kn[c, rows_at, pl.ds((h // per_kv) * head_dim, head_dim)] for h in range(n_head)], axis=0)
            values_new.append(jnp.concatenate([vn[c, rows_at, pl.ds((h // per_kv) * head_dim, head_dim)] for h in range(n_head)], axis=0))
            score_new = jnp.sum(queries[g].astype(F32) * key_new.astype(F32), axis=-1, keepdims=True) * scale
            p_rows = pos[pl.ds(pl.multiple_of(base + g * GROUP, GROUP), GROUP), :]
            p_wide = jnp.concatenate([jnp.concatenate([p_rows] * (keys // p_rows.shape[1]), axis=1)] * n_head, axis=0)
            valid = slot_of < p_wide
            masked = jnp.where(valid, scores[g], -jnp.inf)
            top = jnp.maximum(jnp.max(masked, axis=-1, keepdims=True), score_new)
            exps = jnp.exp(masked - top)
            exp_new = jnp.exp(score_new - top)
            total = jnp.sum(exps, axis=-1, keepdims=True) + exp_new
            probs.append(exps / total)
            probs_new.append((exp_new / total).astype(BF16).astype(F32))
        for g in groups:
            context = None
            for j in range(n_quad):
                val_block = vb[slot, pl.ds(g * GROUP * keys_per_row + j * keys, keys), :]
                one = dot(jnp.where(quad_of == j, probs[g], 0.0).astype(BF16), val_block)
                context = one if context is None else context + one
            context = (context + probs_new[g] * values_new[g].astype(F32)).astype(BF16)
            for h in range(n_head):
                cb[pl.ds(g * GROUP, GROUP), pl.ds(h * head_dim, head_dim)] = context[h * GROUP:(h + 1) * GROUP]

    def attn_part(c):
        @pl.when(c + 1 < N_CHUNK)
        def _():
            for one in load_kv(c + 1, lax.rem(c + 1, 2)):
                one.start()

        attention(c)

        @pl.when(c == 0)
        def _():
            loads[3].wait()

            @pl.when(stage == 0)
            def _():
                for one in loads[4:7]:
                    one.start()
                pl.semaphore_wait(barrier, n_stage * n_tp)

        partials(c, cb[...], wd, o_rows)

        @pl.when(c == N_CHUNK - 1)
        def _():
            loads[7].start()

    def mlp_part(k):
        c = k - N_CHUNK
        add_sum(c)
        nb[...] = norm_rows(hb[c], gain_m[...])

        @pl.when(c == 0)
        def _():
            for one in loads[4:6]:
                one.wait()

        for at, size in column_blocks(wg.shape[1], 512):
            gate = dot(nb[...], wg[:, pl.ds(at, size)]).astype(BF16).astype(F32)
            up = dot(nb[...], wu[:, pl.ds(at, size)]).astype(BF16).astype(F32)
            ab[:, pl.ds(at, size)] = (gate * jax.nn.sigmoid(gate) * up).astype(BF16)

        @pl.when(c == 0)
        def _():
            for one in loads[6:]:
                one.wait()

        wait_part_sends(k - N_CHUNK)
        partials(k, ab[...], wd, wd.shape[0])

    def finish(c):
        add_sum(c)

        @pl.when(stage < n_stage - 1)
        def _():
            remote(hb.at[c], hb.at[c], s_h.at[c], r_h.at[c], stage + 1, line).start()

        @pl.when(stage == n_stage - 1)
        def _():
            hb[c] = norm_rows(hb[c], gain_f[...])
            remote(hb.at[c], out.at[c], s_fwd.at[0, c], r_out.at[c], stage - 2, line).start()
            remote(hb.at[c], out.at[c], s_fwd.at[1, c], r_out.at[c], stage - 1, line).start()
            pltpu.make_async_copy(hb.at[c], out.at[c], s_out.at[c]).start()

    def compute_stage():
        @pl.loop(0, N_CHUNK)
        def _(k):
            attn_part(k)
            relay(k)

        @pl.loop(N_CHUNK, 2 * N_CHUNK)
        def _(k):
            mlp_part(k)
            relay(k)

        @pl.loop(2 * N_CHUNK, 3 * N_CHUNK)
        def _(k):
            finish(k - 2 * N_CHUNK)
            relay(k)

    @pl.when(side == 1)
    def _():
        help_stage()

    compute_stage()

    @pl.when(side == 0)
    def _():
        help_stage()

    @pl.loop(0, N_CHUNK)
    def _(c):
        wait_part_sends(c)
        for i, (ref, dst) in enumerate(((kn, k_out), (vn, v_out))):
            landed(ref.at[c], s_rows.at[i, c])

        @pl.when(is_mid)
        def _():
            for s in range(N_SUB):
                landed(res_a.at[c, s], s_res.at[c, s])
                landed(hres.at[c, s], s_hres0.at[c, s])
                landed(hres.at[c, s], s_hres1.at[c, s])

        @pl.when(is_end)
        def _():
            for s in range(N_SUB):
                landed(hrec0.at[c, s], s_hsum.at[c, s])

        @pl.when(stage < n_stage - 1)
        def _():
            landed(hb.at[c], s_h.at[c])
            landed(out.at[c], r_out.at[c])

        @pl.when(stage == n_stage - 3)
        def _():
            remote(out.at[c], out.at[c], s_fwd.at[0, c], r_out.at[c], stage - 1, line).start()

        @pl.when(stage == n_stage - 1)
        def _():
            landed(hb.at[c], s_out.at[c])
            landed(hb.at[c], s_fwd.at[0, c])
            landed(hb.at[c], s_fwd.at[1, c])

    @pl.when(stage == n_stage - 3)
    def _():
        for c in range(N_CHUNK):
            landed(out.at[c], s_fwd.at[0, c])


def solution(mesh):
    n_stage = mesh.shape['pp']
    n_tp = mesh.shape['tp']
    cache_spec = P('pp', 'dp', None, 'tp', None)
    gain_spec = P('pp', None)
    col_spec = P('pp', None, 'tp')
    row_spec = P('pp', 'tp', None)
    rows_spec = P('pp', 'dp', 'tp', None)

    def stage_fn(hidden_in, positions, k_cache, v_cache, attn_gain, w_q, w_k, w_v, w_o, mlp_gain, w_gate, w_up, w_down, final_gain):
        batch, d_model = hidden_in.shape
        _, _, cache_len, kv_local, head_dim = k_cache.shape
        rows = batch // N_CHUNK
        d_attn = w_q.shape[2]
        kv_width = kv_local * head_dim
        d_ff = w_gate.shape[2]
        half = d_model // 2
        sub = half // N_SUB
        n_head = d_attn // head_dim
        keys = rows * cache_len * kv_local
        score_keys = 4 * cache_len * kv_local
        cos_h, sin_h = rope_tables(positions, head_dim)
        cos_t = jnp.concatenate([cos_h, cos_h], axis=-1)
        sin_t = jnp.concatenate([-sin_h, sin_h], axis=-1)
        pos_wide = jnp.broadcast_to(positions[:, None], (batch, 128))
        anywhere = pl.BlockSpec(memory_space=pl.ANY)
        vmem = pl.BlockSpec(memory_space=pltpu.VMEM)
        dma = pltpu.SemaphoreType.DMA
        blocks = (N_CHUNK, N_SUB)
        call = pl.pallas_call(
            functools.partial(step_kernel, n_stage, n_tp),
            out_shape=[
                jax.ShapeDtypeStruct((N_CHUNK, rows, d_model), BF16),
                jax.ShapeDtypeStruct((N_CHUNK, rows, kv_width), BF16),
                jax.ShapeDtypeStruct((N_CHUNK, rows, kv_width), BF16),
            ],
            in_specs=[anywhere, vmem, vmem, vmem, anywhere, anywhere, vmem] + [anywhere] * 4 + [vmem] + [anywhere] * 3 + [vmem],
            out_specs=[anywhere] * 3,
            scratch_shapes=[
                pltpu.VMEM((d_model, d_attn), BF16),
                pltpu.VMEM((d_model, kv_width), BF16),
                pltpu.VMEM((d_model, kv_width), BF16),
                pltpu.VMEM((d_model, d_ff), BF16),
                pltpu.VMEM((d_model, d_ff), BF16),
                pltpu.VMEM((d_ff, d_model), BF16),
                pltpu.VMEM((2, keys, head_dim), BF16),
                pltpu.VMEM((2, keys, head_dim), BF16),
                pltpu.VMEM((N_CHUNK, rows, d_model), BF16),
                pltpu.VMEM((rows, d_model), BF16),
                pltpu.VMEM((rows, d_attn), BF16),
                pltpu.VMEM((N_CHUNK, rows, kv_width), BF16),
                pltpu.VMEM((N_CHUNK, rows, kv_width), BF16),
                pltpu.VMEM((rows, d_attn), BF16),
                pltpu.VMEM((rows, d_ff), BF16),
                pltpu.VMEM((GROUP * n_head, score_keys), jnp.int32),
                pltpu.VMEM((N_CHUNK, 2 * N_SUB, rows, sub), F32),
                pltpu.VMEM(blocks + (rows, sub), F32),
                pltpu.VMEM((2 * N_CHUNK, N_SUB, rows, sub), F32),
                pltpu.VMEM(blocks + (rows, sub), BF16),
                pltpu.VMEM(blocks + (rows, sub), BF16),
                pltpu.VMEM(blocks + (rows, sub), F32),
                pltpu.VMEM(blocks + (rows, sub), F32),
                pltpu.VMEM((2 * N_CHUNK, N_SUB, rows, sub), F32),
                pltpu.VMEM(blocks + (rows, sub), BF16),
                dma((8,)), dma((2, 2)), dma((2, N_CHUNK)), dma((N_CHUNK,)), dma((2, N_CHUNK)),
                dma((N_CHUNK,)), dma((N_CHUNK,)), dma((N_CHUNK,)),
                dma((N_CHUNK, 2 * N_SUB)), dma(blocks), dma(blocks),
                dma(blocks), dma((2 * N_CHUNK, N_SUB)), dma(blocks), dma(blocks),
                dma(blocks), dma(blocks), dma(blocks), dma(blocks), dma(blocks), dma((2 * N_CHUNK, N_SUB)),
            ],
            compiler_params=pltpu.CompilerParams(collective_id=0, has_side_effects=True, vmem_limit_bytes=67043328),
        )
        out, k_rows, v_rows = call(
            hidden_in.reshape(N_CHUNK, rows, d_model), pos_wide, cos_t, sin_t,
            k_cache.reshape(N_CHUNK, keys, head_dim), v_cache.reshape(N_CHUNK, keys, head_dim),
            attn_gain, w_q[0], w_k[0], w_v[0], w_o[0], mlp_gain, w_gate[0], w_up[0], w_down[0], final_gain[None])
        shape = (1, batch, kv_local, head_dim)
        return out.reshape(batch, d_model), k_rows.reshape(shape), v_rows.reshape(shape)

    return jax.shard_map(
        stage_fn,
        mesh=mesh,
        in_specs=(P('dp', None), P('dp'), cache_spec, cache_spec, gain_spec, col_spec, col_spec, col_spec, row_spec, gain_spec, col_spec, col_spec, row_spec, P(None)),
        out_specs=(P('dp', None), rows_spec, rows_spec),
        check_vma=False,
    )
```

```python
import functools

import jax
import jax.numpy as jnp
import numpy as np
from jax import lax
from jax.experimental import pallas as pl
from jax.experimental.pallas import tpu as pltpu
from jax.sharding import PartitionSpec as P

RMS_EPS = 1e-5
ROPE_THETA = 500000.0
BF16 = jnp.bfloat16
F32 = jnp.float32
MESH = pl.DeviceIdType.MESH

N_CHUNK = 4
N_A = 6
N_B = 4
GROUP = 16


def norm_rows(rows, gain):
    rows32 = rows.astype(F32)
    mean_sq = jnp.mean(rows32 * rows32, axis=-1, keepdims=True)
    return (rows32 * lax.rsqrt(mean_sq + RMS_EPS) * gain.astype(F32)).astype(BF16)


def dot(a, b):
    return jnp.dot(a, b, preferred_element_type=F32)


def column_blocks(width, size):
    return [(at, min(size, width - at)) for at in range(0, width, size)]


def step_kernel(
    n_stage, n_tp,
    hid, pos_row, inv_freq, k_hbm, v_hbm, gain_a, w_q, w_k, w_v, w_o, gain_m, w_g, w_u, w_d, gain_f,
    out, k_out, v_out,
    wq, wk, wv, wg, wu, wd, kb, vb, hb, nb, qb, kn, vn, ko, vo, mix, cb, ab, slots, pos, cos_t, sin_t,
    part, rec_e, rec_m, res_a, res_b, hrec0, hrec1, hres,
    s_w, s_kv, s_rows, s_out, s_fwd,
    r_h, s_h, r_out, s_part, s_sum, s_res, s_res2, r_e, r_m, r_a, r_b,
    s_hsum, s_hres0, s_hres1, r_h0, r_h1, r_hm,
):
    rows = hb.shape[1]
    sub = part.shape[3]
    d_attn = cb.shape[1]
    kv_width = kn.shape[2]
    head_dim = kb.shape[2]
    n_head = d_attn // head_dim
    kv_heads = kv_width // head_dim
    per_kv = n_head // kv_heads
    cache_len = kb.shape[1] // (rows * kv_heads)
    stage = lax.axis_index('pp')
    line = lax.axis_index('tp')
    side = stage // 2
    helped = lax.rem(stage + 2, n_stage)
    is_mid = jnp.logical_or(line == 1, line == n_tp - 2)
    is_end = jnp.logical_not(is_mid)
    mid_of = jnp.where(line < n_tp // 2, 1, n_tp - 2)
    end_of = jnp.where(line < n_tp // 2, 0, n_tp - 1)
    other_mid = n_tp - 1 - line

    def remote(src, dst, send, recv, to_stage, to_line):
        return pltpu.make_async_remote_copy(
            src_ref=src, dst_ref=dst, send_sem=send, recv_sem=recv,
            device_id={'pp': to_stage, 'tp': to_line}, device_id_type=MESH)

    def landed(ref, sem):
        pltpu.make_async_copy(ref, ref, sem).wait()

    barrier = pltpu.get_barrier_semaphore()
    for other_stage in range(n_stage):
        for other_line in range(n_tp):
            pl.semaphore_signal(barrier, inc=1, device_id={'pp': other_stage, 'tp': other_line}, device_id_type=MESH)

    @pl.when(stage == 0)
    def _():
        for c in range(N_CHUNK):
            pltpu.make_async_copy(hid.at[c], hb.at[c], r_h.at[c]).start()

    def load_kv(c, slot):
        return (pltpu.make_async_copy(k_hbm.at[c], kb.at[slot], s_kv.at[0, slot]),
                pltpu.make_async_copy(v_hbm.at[c], vb.at[slot], s_kv.at[1, slot]))

    o_rows = w_o.shape[0]
    loads = [
        pltpu.make_async_copy(w_q, wq, s_w.at[0]),
        pltpu.make_async_copy(w_k, wk, s_w.at[1]),
        pltpu.make_async_copy(w_v, wv, s_w.at[2]),
        pltpu.make_async_copy(w_o, wd.at[pl.ds(0, o_rows)], s_w.at[3]),
        pltpu.make_async_copy(w_g, wg, s_w.at[4]),
        pltpu.make_async_copy(w_u, wu, s_w.at[5]),
        pltpu.make_async_copy(w_d.at[pl.ds(o_rows, w_d.shape[0] - o_rows)], wd.at[pl.ds(o_rows, w_d.shape[0] - o_rows)], s_w.at[6]),
        pltpu.make_async_copy(w_d.at[pl.ds(0, o_rows)], wd.at[pl.ds(0, o_rows)], s_w.at[7]),
    ]
    for one in loads[:3]:
        one.start()
    for one in load_kv(0, 0):
        one.start()
    loads[3].start()

    @pl.when(stage > 0)
    def _():
        for one in loads[4:7]:
            one.start()
        pl.semaphore_wait(barrier, n_stage * n_tp)

    row_id = lax.broadcasted_iota(jnp.int32, slots.shape, 0)
    col_id = lax.broadcasted_iota(jnp.int32, slots.shape, 1)
    keys_per_row = cache_len * kv_heads
    quad = slots.shape[1] // keys_per_row
    same_row = lax.rem(row_id, quad) == col_id // keys_per_row
    same_head = lax.rem(col_id, kv_heads) == row_id // (GROUP * per_kv)
    slots[...] = jnp.where(jnp.logical_and(same_row, same_head), lax.rem(col_id, keys_per_row) // kv_heads, cache_len)

    square = (128, 128)
    on_diag = lax.broadcasted_iota(jnp.int32, square, 0) == lax.broadcasted_iota(jnp.int32, square, 1)
    first_half = lax.broadcasted_iota(jnp.int32, square, 1) < head_dim // 2
    for b in range(pos_row.shape[0]):
        wide = jnp.where(on_diag, jnp.broadcast_to(pos_row[pl.ds(b, 1), :], square), 0).astype(F32)
        column = jnp.broadcast_to(jnp.sum(wide, axis=1, keepdims=True), square)
        at = pl.ds(b * 128, 128)
        pos[at, :] = column.astype(jnp.int32)
        angles = column * inv_freq[...]
        cos_t[at, :] = jnp.cos(angles)
        sines = jnp.sin(angles)
        sin_t[at, :] = jnp.where(first_half, -sines, sines)

    def send_part(k, b_half):
        kc = lax.rem(k, N_CHUNK)
        if b_half:
            @pl.when(is_end)
            def _():
                for s in range(N_B):
                    remote(part.at[kc, N_A + s], rec_m.at[k, s], s_part.at[kc, N_A + s], r_hm.at[k, s], helped, line).start()

            @pl.when(is_mid)
            def _():
                for s in range(N_B):
                    remote(part.at[kc, N_A + s], hrec1.at[kc, s], s_part.at[kc, N_A + s], r_h1.at[kc, s], helped, line).start()
        else:
            @pl.when(is_end)
            def _():
                for s in range(N_A):
                    remote(part.at[kc, s], rec_e.at[kc, s], s_part.at[kc, s], r_e.at[kc, s], stage, mid_of).start()

    def wait_part_sends(k):
        kc = lax.rem(k, N_CHUNK)
        for s in range(N_B):
            landed(part.at[kc, N_A + s], s_part.at[kc, N_A + s])

        @pl.when(is_end)
        def _():
            for s in range(N_A):
                landed(part.at[kc, s], s_part.at[kc, s])

        @pl.when(is_mid)
        def _():
            for s in range(N_A):
                landed(part.at[kc, s], s_sum.at[kc, s])

    def sum_first(k):
        kc = lax.rem(k, N_CHUNK)
        for s in range(N_A):
            landed(rec_e.at[kc, s], r_e.at[kc, s])
            part[kc, s] = part[kc, s] + rec_e[kc, s]
            remote(part.at[kc, s], rec_m.at[k, s], s_sum.at[kc, s], r_m.at[k, s], stage, other_mid).start()

    def sum_second(k):
        kc = lax.rem(k, N_CHUNK)
        to_stage = jnp.where(k < N_CHUNK, stage, jnp.minimum(stage + 1, n_stage - 1))

        @pl.when(k >= N_CHUNK)
        def _():
            for s in range(N_A):
                landed(res_a.at[kc, s], s_res.at[kc, s])

        for s in range(N_A):
            landed(rec_m.at[k, s], r_m.at[k, s])
            res_a[k, s] = (part[kc, s] + rec_m[k, s]).astype(BF16)
            remote(res_a.at[k, s], res_a.at[k, s], s_res.at[kc, s], r_a.at[k, s], to_stage, end_of).start()

            @pl.when(jnp.logical_and(k >= N_CHUNK, stage < n_stage - 1))
            def _():
                remote(res_a.at[k, s], res_a.at[k, s], s_res2.at[kc, s], r_a.at[k, s], to_stage, line).start()

    def help_first(k):
        kc = lax.rem(k, N_CHUNK)
        for s in range(N_B):
            landed(hrec0.at[kc, s], r_h0.at[kc, s])
            landed(hrec1.at[kc, s], r_h1.at[kc, s])
            hrec1[kc, s] = hrec1[kc, s] + hrec0[kc, s]
            remote(hrec1.at[kc, s], rec_m.at[k, s], s_hsum.at[kc, s], r_hm.at[k, s], stage, other_mid).start()

    def help_second(k):
        kc = lax.rem(k, N_CHUNK)
        to_stage = jnp.where(k < N_CHUNK, helped, jnp.minimum(helped + 1, n_stage - 1))

        @pl.when(k >= N_CHUNK)
        def _():
            for s in range(N_B):
                landed(hres.at[kc, s], s_hres0.at[kc, s])
                landed(hres.at[kc, s], s_hres1.at[kc, s])

        for s in range(N_B):
            landed(rec_m.at[k, s], r_hm.at[k, s])
            landed(hrec1.at[kc, s], s_hsum.at[kc, s])
            hres[kc, s] = (hrec1[kc, s] + rec_m[k, s]).astype(BF16)
            remote(hres.at[kc, s], res_b.at[k, s], s_hres0.at[kc, s], r_b.at[k, s], to_stage, end_of).start()
            remote(hres.at[kc, s], res_b.at[k, s], s_hres1.at[kc, s], r_b.at[k, s], to_stage, line).start()

    def help_forward(k):
        kc = lax.rem(k, N_CHUNK)

        @pl.when(k >= N_CHUNK)
        def _():
            for s in range(N_B):
                landed(hrec0.at[kc, s], s_hsum.at[kc, s])

        for s in range(N_B):
            landed(rec_m.at[k, s], r_hm.at[k, s])
            remote(rec_m.at[k, s], hrec0.at[kc, s], s_hsum.at[kc, s], r_h0.at[kc, s], stage, mid_of).start()

    def help_stage():
        @pl.when(is_end)
        def _():
            @pl.loop(0, 2 * N_CHUNK)
            def _(k):
                help_forward(k)

        @pl.when(is_mid)
        def _():
            @pl.loop(0, 2 * N_CHUNK + 1)
            def _(k):
                @pl.when(k < 2 * N_CHUNK)
                def _():
                    help_first(k)

                @pl.when(k >= 1)
                def _():
                    help_second(k - 1)

    def relay(k):
        @pl.when(is_mid)
        def _():
            @pl.when(jnp.logical_and(k >= 1, k <= 2 * N_CHUNK))
            def _():
                sum_first(k - 1)

            @pl.when(jnp.logical_and(k >= 2, k <= 2 * N_CHUNK + 1))
            def _():
                sum_second(k - 2)

    def add_sum(c, k, remote_a):
        @pl.when(remote_a)
        def _():
            for s in range(N_A):
                landed(res_a.at[k, s], r_a.at[k, s])

        for s in range(N_A):
            at = pl.ds(s * sub, sub)
            hb[c, :, at] = (hb[c, :, at].astype(F32) + res_a[k, s].astype(F32)).astype(BF16)
        for s in range(N_B):
            at = pl.ds((N_A + s) * sub, sub)
            landed(res_b.at[k, s], r_b.at[k, s])
            hb[c, :, at] = (hb[c, :, at].astype(F32) + res_b[k, s].astype(F32)).astype(BF16)

    def partials(k, act, weight, depth):
        kc = lax.rem(k, N_CHUNK)
        for b_half in (True, False):
            base, count = (N_A, N_B) if b_half else (0, N_A)
            got = dot(act, weight[pl.ds(0, depth), pl.ds(base * sub, count * sub)])
            for s in range(count):
                part[kc, base + s] = got[:, s * sub:(s + 1) * sub]
            send_part(k, b_half)

    def attention(c):
        slot = lax.rem(c, 2)
        landed(hb.at[c], r_h.at[c])

        @pl.when(stage > 0)
        def _():
            add_sum(c, N_CHUNK + c, stage > 0)

        @pl.when(c == 0)
        def _():
            for one in loads[:3]:
                one.wait()

        normed = norm_rows(hb[c], gain_a[...])
        base = pl.multiple_of(c * rows, rows)
        cosv = cos_t[pl.ds(base, rows), :]
        sinv = sin_t[pl.ds(base, rows), :]

        def rope(vals):
            vals32 = vals.astype(BF16).astype(F32)
            return (vals32 * cosv + pltpu.roll(vals32, head_dim // 2, 1) * sinv).astype(BF16)

        nb[...] = normed
        got_k = dot(nb[...], wk[...])
        got_v = dot(nb[...], wv[...])
        for g in range(kv_heads):
            at = pl.ds(g * head_dim, head_dim)
            rotated = rope(got_k[:, g * head_dim:(g + 1) * head_dim])
            kn[c, :, at] = rotated
            mix[0, pl.ds(g, rows, stride=kv_heads), :] = rotated.astype(F32)
            mix[1, pl.ds(g, rows, stride=kv_heads), :] = got_v[:, g * head_dim:(g + 1) * head_dim]
        vn[c] = got_v.astype(BF16)
        ko[c] = mix[0].astype(BF16)
        vo[c] = mix[1].astype(BF16)
        pltpu.make_async_copy(ko.at[c], k_out.at[c], s_rows.at[0, c]).start()
        pltpu.make_async_copy(vo.at[c], v_out.at[c], s_rows.at[1, c]).start()
        got_q = dot(nb[...], wq[...])
        for h in range(n_head):
            qb[:, pl.ds(h * head_dim, head_dim)] = rope(got_q[:, h * head_dim:(h + 1) * head_dim])

        for one in load_kv(c, slot):
            one.wait()
        scale = head_dim ** -0.5
        keys = slots.shape[1]
        n_quad = GROUP // quad
        rows_id = lax.broadcasted_iota(jnp.int32, (GROUP * n_head, keys), 0)
        quad_of = lax.rem(rows_id, GROUP) // quad
        slot_of = slots[...]
        groups = range(rows // GROUP)
        queries = []
        scores = []
        for g in groups:
            rows_at = pl.ds(g * GROUP, GROUP)
            queries.append(jnp.concatenate([qb[rows_at, pl.ds(h * head_dim, head_dim)] for h in range(n_head)], axis=0))
            picked = None
            for j in range(n_quad):
                key_block = kb[slot, pl.ds(g * GROUP * keys_per_row + j * keys, keys), :]
                one = lax.dot_general(queries[g], key_block, (((1,), (1,)), ((), ())), preferred_element_type=F32)
                picked = one if picked is None else jnp.where(quad_of == j, one, picked)
            scores.append(picked * scale)
        probs = []
        probs_new = []
        values_new = []
        for g in groups:
            rows_at = pl.ds(g * GROUP, GROUP)
            key_new = jnp.concatenate([kn[c, rows_at, pl.ds((h // per_kv) * head_dim, head_dim)] for h in range(n_head)], axis=0)
            values_new.append(jnp.concatenate([vn[c, rows_at, pl.ds((h // per_kv) * head_dim, head_dim)] for h in range(n_head)], axis=0))
            score_new = jnp.sum(queries[g].astype(F32) * key_new.astype(F32), axis=-1, keepdims=True) * scale
            p_rows = pos[pl.ds(pl.multiple_of(base + g * GROUP, GROUP), GROUP), :]
            p_wide = jnp.concatenate([jnp.concatenate([p_rows] * (keys // p_rows.shape[1]), axis=1)] * n_head, axis=0)
            valid = slot_of < p_wide
            masked = jnp.where(valid, scores[g], -jnp.inf)
            top = jnp.maximum(jnp.max(masked, axis=-1, keepdims=True), score_new)
            exps = jnp.exp(masked - top)
            exp_new = jnp.exp(score_new - top)
            total = jnp.sum(exps, axis=-1, keepdims=True) + exp_new
            probs.append(exps / total)
            probs_new.append((exp_new / total).astype(BF16).astype(F32))
        for g in groups:
            context = None
            for j in range(n_quad):
                val_block = vb[slot, pl.ds(g * GROUP * keys_per_row + j * keys, keys), :]
                one = dot(jnp.where(quad_of == j, probs[g], 0.0).astype(BF16), val_block)
                context = one if context is None else context + one
            context = (context + probs_new[g] * values_new[g].astype(F32)).astype(BF16)
            for h in range(n_head):
                cb[pl.ds(g * GROUP, GROUP), pl.ds(h * head_dim, head_dim)] = context[h * GROUP:(h + 1) * GROUP]

    def attn_part(c):
        @pl.when(c + 1 < N_CHUNK)
        def _():
            for one in load_kv(c + 1, lax.rem(c + 1, 2)):
                one.start()

        attention(c)

        @pl.when(c == 0)
        def _():
            loads[3].wait()

            @pl.when(stage == 0)
            def _():
                for one in loads[4:7]:
                    one.start()
                pl.semaphore_wait(barrier, n_stage * n_tp)

        partials(c, cb[...], wd, o_rows)

        @pl.when(c == N_CHUNK - 1)
        def _():
            loads[7].start()

    def mlp_part(k):
        c = k - N_CHUNK
        add_sum(c, c, is_end)
        nb[...] = norm_rows(hb[c], gain_m[...])

        @pl.when(c == 0)
        def _():
            for one in loads[4:6]:
                one.wait()

        for at, size in column_blocks(wg.shape[1], 512):
            gate = dot(nb[...], wg[:, pl.ds(at, size)]).astype(BF16).astype(F32)
            up = dot(nb[...], wu[:, pl.ds(at, size)]).astype(BF16).astype(F32)
            ab[:, pl.ds(at, size)] = (gate * jax.nn.sigmoid(gate) * up).astype(BF16)

        @pl.when(c == 0)
        def _():
            for one in loads[6:]:
                one.wait()

        wait_part_sends(k - N_CHUNK)
        partials(k, ab[...], wd, wd.shape[0])

        @pl.when(stage < n_stage - 1)
        def _():
            remote(hb.at[c], hb.at[c], s_h.at[c], r_h.at[c], stage + 1, line).start()

    def finish(c):
        @pl.when(stage == n_stage - 1)
        def _():
            add_sum(c, N_CHUNK + c, is_end)
            hb[c] = norm_rows(hb[c], gain_f[...].reshape(1, hb.shape[2]))
            remote(hb.at[c], out.at[c], s_fwd.at[0, c], r_out.at[c], stage - 2, line).start()
            remote(hb.at[c], out.at[c], s_fwd.at[1, c], r_out.at[c], stage - 1, line).start()
            pltpu.make_async_copy(hb.at[c], out.at[c], s_out.at[c]).start()

    def compute_stage():
        @pl.loop(0, N_CHUNK)
        def _(k):
            attn_part(k)
            relay(k)

        @pl.loop(N_CHUNK, 2 * N_CHUNK)
        def _(k):
            mlp_part(k)
            relay(k)

        @pl.loop(2 * N_CHUNK, 3 * N_CHUNK)
        def _(k):
            finish(k - 2 * N_CHUNK)
            relay(k)

    @pl.when(side == 1)
    def _():
        help_stage()

    compute_stage()

    @pl.when(side == 0)
    def _():
        help_stage()

    @pl.loop(0, N_CHUNK)
    def _(c):
        wait_part_sends(c)
        for i, (ref, dst) in enumerate(((ko, k_out), (vo, v_out))):
            landed(ref.at[c], s_rows.at[i, c])

        @pl.when(is_mid)
        def _():
            for s in range(N_A):
                landed(res_a.at[c, s], s_res.at[c, s])

            @pl.when(stage < n_stage - 1)
            def _():
                for s in range(N_A):
                    landed(res_a.at[c, s], s_res2.at[c, s])

            for s in range(N_B):
                landed(hres.at[c, s], s_hres0.at[c, s])
                landed(hres.at[c, s], s_hres1.at[c, s])

        @pl.when(is_end)
        def _():
            for s in range(N_B):
                landed(hrec0.at[c, s], s_hsum.at[c, s])

        @pl.when(stage < n_stage - 1)
        def _():
            landed(hb.at[c], s_h.at[c])
            landed(out.at[c], r_out.at[c])

        @pl.when(stage == n_stage - 3)
        def _():
            remote(out.at[c], out.at[c], s_fwd.at[0, c], r_out.at[c], stage - 1, line).start()

        @pl.when(stage == n_stage - 1)
        def _():
            landed(hb.at[c], s_out.at[c])
            landed(hb.at[c], s_fwd.at[0, c])
            landed(hb.at[c], s_fwd.at[1, c])

    @pl.when(stage == n_stage - 3)
    def _():
        for c in range(N_CHUNK):
            landed(out.at[c], s_fwd.at[0, c])


def solution(mesh):
    n_stage = mesh.shape['pp']
    n_tp = mesh.shape['tp']
    cache_spec = P('pp', 'dp', None, 'tp', None)
    gain_spec = P('pp', None)
    col_spec = P('pp', None, 'tp')
    row_spec = P('pp', 'tp', None)
    rows_spec = P('pp', 'dp', 'tp', None)

    def stage_fn(hidden_in, positions, k_cache, v_cache, attn_gain, w_q, w_k, w_v, w_o, mlp_gain, w_gate, w_up, w_down, final_gain):
        batch, d_model = hidden_in.shape
        _, _, cache_len, kv_local, head_dim = k_cache.shape
        rows = batch // N_CHUNK
        d_attn = w_q.shape[2]
        kv_width = kv_local * head_dim
        d_ff = w_gate.shape[2]
        sub = d_model // (N_A + N_B)
        n_head = d_attn // head_dim
        keys = rows * cache_len * kv_local
        score_keys = 4 * cache_len * kv_local
        inverse = ROPE_THETA ** (-np.arange(0, head_dim, 2).astype(np.float32) / head_dim)
        inv_freq = jnp.asarray(np.concatenate([inverse, inverse])[None].astype(np.float32))
        anywhere = pl.BlockSpec(memory_space=pl.ANY)
        vmem = pl.BlockSpec(memory_space=pltpu.VMEM)
        dma = pltpu.SemaphoreType.DMA
        a_blocks = (N_CHUNK, N_A)
        b_blocks = (N_CHUNK, N_B)
        tile = (rows, sub)
        call = pl.pallas_call(
            functools.partial(step_kernel, n_stage, n_tp),
            out_shape=[
                jax.ShapeDtypeStruct((N_CHUNK, rows, d_model), BF16),
                jax.ShapeDtypeStruct((N_CHUNK, rows * kv_local, head_dim), BF16),
                jax.ShapeDtypeStruct((N_CHUNK, rows * kv_local, head_dim), BF16),
            ],
            in_specs=[anywhere, vmem, vmem, anywhere, anywhere, vmem] + [anywhere] * 4 + [vmem] + [anywhere] * 3 + [vmem],
            out_specs=[anywhere] * 3,
            scratch_shapes=[
                pltpu.VMEM((d_model, d_attn), BF16),
                pltpu.VMEM((d_model, kv_width), BF16),
                pltpu.VMEM((d_model, kv_width), BF16),
                pltpu.VMEM((d_model, d_ff), BF16),
                pltpu.VMEM((d_model, d_ff), BF16),
                pltpu.VMEM((d_ff, d_model), BF16),
                pltpu.VMEM((2, keys, head_dim), BF16),
                pltpu.VMEM((2, keys, head_dim), BF16),
                pltpu.VMEM((N_CHUNK, rows, d_model), BF16),
                pltpu.VMEM((rows, d_model), BF16),
                pltpu.VMEM((rows, d_attn), BF16),
                pltpu.VMEM((N_CHUNK, rows, kv_width), BF16),
                pltpu.VMEM((N_CHUNK, rows, kv_width), BF16),
                pltpu.VMEM((N_CHUNK, rows * kv_local, head_dim), BF16),
                pltpu.VMEM((N_CHUNK, rows * kv_local, head_dim), BF16),
                pltpu.VMEM((2, rows * kv_local, head_dim), F32),
                pltpu.VMEM((rows, d_attn), BF16),
                pltpu.VMEM((rows, d_ff), BF16),
                pltpu.VMEM((GROUP * n_head, score_keys), jnp.int32),
                pltpu.VMEM((batch, 128), jnp.int32),
                pltpu.VMEM((batch, head_dim), F32),
                pltpu.VMEM((batch, head_dim), F32),
                pltpu.VMEM((N_CHUNK, N_A + N_B) + tile, F32),
                pltpu.VMEM(a_blocks + tile, F32),
                pltpu.VMEM((2 * N_CHUNK, max(N_A, N_B)) + tile, F32),
                pltpu.VMEM((2 * N_CHUNK, N_A) + tile, BF16),
                pltpu.VMEM((2 * N_CHUNK, N_B) + tile, BF16),
                pltpu.VMEM(b_blocks + tile, F32),
                pltpu.VMEM(b_blocks + tile, F32),
                pltpu.VMEM(b_blocks + tile, BF16),
                dma((8,)), dma((2, 2)), dma((2, N_CHUNK)), dma((N_CHUNK,)), dma((2, N_CHUNK)),
                dma((N_CHUNK,)), dma((N_CHUNK,)), dma((N_CHUNK,)),
                dma((N_CHUNK, N_A + N_B)), dma(a_blocks), dma(a_blocks), dma(a_blocks),
                dma(a_blocks), dma((2 * N_CHUNK, N_A)), dma((2 * N_CHUNK, N_A)), dma((2 * N_CHUNK, N_B)),
                dma(b_blocks), dma(b_blocks), dma(b_blocks), dma(b_blocks), dma(b_blocks), dma((2 * N_CHUNK, N_B)),
            ],
            compiler_params=pltpu.CompilerParams(collective_id=0, has_side_effects=True, vmem_limit_bytes=67043328),
        )
        out, k_rows, v_rows = call(
            hidden_in.reshape(N_CHUNK, rows, d_model), positions.reshape(-1, 128), inv_freq,
            k_cache.reshape(N_CHUNK, keys, head_dim), v_cache.reshape(N_CHUNK, keys, head_dim),
            attn_gain, w_q[0], w_k[0], w_v[0], w_o[0], mlp_gain, w_gate[0], w_up[0], w_down[0], final_gain)
        shape = (1, batch, kv_local, head_dim)
        return out.reshape(batch, d_model), k_rows.reshape(shape), v_rows.reshape(shape)

    return jax.shard_map(
        stage_fn,
        mesh=mesh,
        in_specs=(P('dp', None), P('dp'), cache_spec, cache_spec, gain_spec, col_spec, col_spec, col_spec, row_spec, gain_spec, col_spec, col_spec, row_spec, P(None)),
        out_specs=(P('dp', None), rows_spec, rows_spec),
        check_vma=False,
    )
```

```python
import functools

import jax
import jax.numpy as jnp
import numpy as np
from jax import lax
from jax.experimental import pallas as pl
from jax.experimental.pallas import tpu as pltpu
from jax.sharding import PartitionSpec as P

RMS_EPS = 1e-5
ROPE_THETA = 500000.0
BF16 = jnp.bfloat16
F32 = jnp.float32
MESH = pl.DeviceIdType.MESH

N_CHUNK = 4
N_A = 5
N_B = 5
GROUP = 16


def norm_rows(rows, gain):
    rows32 = rows.astype(F32)
    mean_sq = jnp.mean(rows32 * rows32, axis=-1, keepdims=True)
    return (rows32 * lax.rsqrt(mean_sq + RMS_EPS) * gain.astype(F32)).astype(BF16)


def dot(a, b):
    return jnp.dot(a, b, preferred_element_type=F32)


def column_blocks(width, size):
    return [(at, min(size, width - at)) for at in range(0, width, size)]


def step_kernel(
    n_stage, n_tp,
    hid, pos_row, inv_freq, k_hbm, v_hbm, gain_a, w_q, w_k, w_v, w_o, gain_m, w_g, w_u, w_d, gain_f,
    out, k_out, v_out,
    wq, wk, wv, wg, wu, wd, kb, vb, hb, nb, qb, kn, vn, ko, vo, mix, cb, ab, slots, pos, cos_t, sin_t,
    part, rec_e, rec_m, res_a, res_b, hrec0, hrec1, hres,
    s_w, s_kv, s_rows, s_out, s_fwd,
    r_h, s_h, r_out, s_part, s_sum, s_res, s_res2, s_res3, r_e, r_m, r_a, r_b,
    s_hsum, s_hres0, s_hres1, s_hres2, r_h0, r_h1, r_hm,
):
    rows = hb.shape[1]
    sub = part.shape[3]
    d_attn = cb.shape[1]
    kv_width = kn.shape[2]
    head_dim = kb.shape[2]
    n_head = d_attn // head_dim
    kv_heads = kv_width // head_dim
    per_kv = n_head // kv_heads
    cache_len = kb.shape[1] // (rows * kv_heads)
    stage = lax.axis_index('pp')
    line = lax.axis_index('tp')
    side = stage // 2
    helped = lax.rem(stage + 2, n_stage)
    is_mid = jnp.logical_or(line == 1, line == n_tp - 2)
    is_end = jnp.logical_not(is_mid)
    mid_of = jnp.where(line < n_tp // 2, 1, n_tp - 2)
    end_of = jnp.where(line < n_tp // 2, 0, n_tp - 1)
    other_mid = n_tp - 1 - line
    last = n_stage - 1
    mirror = last - 2
    after = jnp.where(stage < last, stage + 1, mirror)

    def remote(src, dst, send, recv, to_stage, to_line):
        return pltpu.make_async_remote_copy(
            src_ref=src, dst_ref=dst, send_sem=send, recv_sem=recv,
            device_id={'pp': to_stage, 'tp': to_line}, device_id_type=MESH)

    def landed(ref, sem):
        pltpu.make_async_copy(ref, ref, sem).wait()

    barrier = pltpu.get_barrier_semaphore()
    for other_stage in range(n_stage):
        for other_line in range(n_tp):
            pl.semaphore_signal(barrier, inc=1, device_id={'pp': other_stage, 'tp': other_line}, device_id_type=MESH)

    @pl.when(stage == 0)
    def _():
        for c in range(N_CHUNK):
            pltpu.make_async_copy(hid.at[c], hb.at[c], r_h.at[c]).start()

    def load_kv(c, slot):
        return (pltpu.make_async_copy(k_hbm.at[c], kb.at[slot], s_kv.at[0, slot]),
                pltpu.make_async_copy(v_hbm.at[c], vb.at[slot], s_kv.at[1, slot]))

    o_rows = w_o.shape[0]
    loads = [
        pltpu.make_async_copy(w_q, wq, s_w.at[0]),
        pltpu.make_async_copy(w_k, wk, s_w.at[1]),
        pltpu.make_async_copy(w_v, wv, s_w.at[2]),
        pltpu.make_async_copy(w_o, wd.at[pl.ds(0, o_rows)], s_w.at[3]),
        pltpu.make_async_copy(w_g, wg, s_w.at[4]),
        pltpu.make_async_copy(w_u, wu, s_w.at[5]),
        pltpu.make_async_copy(w_d.at[pl.ds(o_rows, w_d.shape[0] - o_rows)], wd.at[pl.ds(o_rows, w_d.shape[0] - o_rows)], s_w.at[6]),
        pltpu.make_async_copy(w_d.at[pl.ds(0, o_rows)], wd.at[pl.ds(0, o_rows)], s_w.at[7]),
    ]
    for one in loads[:3]:
        one.start()
    for one in load_kv(0, 0):
        one.start()
    loads[3].start()

    @pl.when(stage > 0)
    def _():
        for one in loads[4:7]:
            one.start()
        pl.semaphore_wait(barrier, n_stage * n_tp)

    row_id = lax.broadcasted_iota(jnp.int32, slots.shape, 0)
    col_id = lax.broadcasted_iota(jnp.int32, slots.shape, 1)
    keys_per_row = cache_len * kv_heads
    quad = slots.shape[1] // keys_per_row
    same_row = lax.rem(row_id, quad) == col_id // keys_per_row
    same_head = lax.rem(col_id, kv_heads) == row_id // (GROUP * per_kv)
    slots[...] = jnp.where(jnp.logical_and(same_row, same_head), lax.rem(col_id, keys_per_row) // kv_heads, cache_len)

    square = (128, 128)
    on_diag = lax.broadcasted_iota(jnp.int32, square, 0) == lax.broadcasted_iota(jnp.int32, square, 1)
    first_half = lax.broadcasted_iota(jnp.int32, square, 1) < head_dim // 2
    for b in range(pos_row.shape[0]):
        wide = jnp.where(on_diag, jnp.broadcast_to(pos_row[pl.ds(b, 1), :], square), 0).astype(F32)
        column = jnp.broadcast_to(jnp.sum(wide, axis=1, keepdims=True), square)
        at = pl.ds(b * 128, 128)
        pos[at, :] = column.astype(jnp.int32)
        angles = column * inv_freq[...]
        cos_t[at, :] = jnp.cos(angles)
        sines = jnp.sin(angles)
        sin_t[at, :] = jnp.where(first_half, -sines, sines)

    def send_part(k, b_half):
        kc = lax.rem(k, N_CHUNK)
        if b_half:
            @pl.when(is_end)
            def _():
                for s in range(N_B):
                    remote(part.at[kc, N_A + s], rec_m.at[k, s], s_part.at[kc, N_A + s], r_hm.at[k, s], helped, line).start()

            @pl.when(is_mid)
            def _():
                for s in range(N_B):
                    remote(part.at[kc, N_A + s], hrec1.at[kc, s], s_part.at[kc, N_A + s], r_h1.at[kc, s], helped, line).start()
        else:
            @pl.when(is_end)
            def _():
                for s in range(N_A):
                    remote(part.at[kc, s], rec_e.at[kc, s], s_part.at[kc, s], r_e.at[kc, s], stage, mid_of).start()

    def wait_part_sends(k):
        kc = lax.rem(k, N_CHUNK)
        for s in range(N_B):
            landed(part.at[kc, N_A + s], s_part.at[kc, N_A + s])

        @pl.when(is_end)
        def _():
            for s in range(N_A):
                landed(part.at[kc, s], s_part.at[kc, s])

        @pl.when(is_mid)
        def _():
            for s in range(N_A):
                landed(part.at[kc, s], s_sum.at[kc, s])

    def sum_first(k):
        kc = lax.rem(k, N_CHUNK)
        for s in range(N_A):
            landed(rec_e.at[kc, s], r_e.at[kc, s])
            part[kc, s] = part[kc, s] + rec_e[kc, s]
            remote(part.at[kc, s], rec_m.at[k, s], s_sum.at[kc, s], r_m.at[k, s], stage, other_mid).start()

    def sum_second(k):
        kc = lax.rem(k, N_CHUNK)
        to_stage = jnp.where(k < N_CHUNK, stage, jnp.minimum(stage + 1, n_stage - 1))

        @pl.when(k >= N_CHUNK)
        def _():
            for s in range(N_A):
                landed(res_a.at[kc, s], s_res.at[kc, s])

        for s in range(N_A):
            landed(rec_m.at[k, s], r_m.at[k, s])
            res_a[k, s] = (part[kc, s] + rec_m[k, s]).astype(BF16)
            remote(res_a.at[k, s], res_a.at[k, s], s_res.at[kc, s], r_a.at[k, s], to_stage, end_of).start()

            @pl.when(k >= N_CHUNK)
            def _():
                remote(res_a.at[k, s], res_a.at[k, s], s_res2.at[kc, s], r_a.at[k, s], after, line).start()

            @pl.when(jnp.logical_and(k >= N_CHUNK, stage == last))
            def _():
                remote(res_a.at[k, s], res_a.at[k, s], s_res3.at[kc, s], r_a.at[k, s], after, end_of).start()

    def help_first(k):
        kc = lax.rem(k, N_CHUNK)
        for s in range(N_B):
            landed(hrec0.at[kc, s], r_h0.at[kc, s])
            landed(hrec1.at[kc, s], r_h1.at[kc, s])
            hrec1[kc, s] = hrec1[kc, s] + hrec0[kc, s]
            remote(hrec1.at[kc, s], rec_m.at[k, s], s_hsum.at[kc, s], r_hm.at[k, s], stage, other_mid).start()

    def help_second(k):
        kc = lax.rem(k, N_CHUNK)
        to_stage = jnp.where(k < N_CHUNK, helped, jnp.minimum(helped + 1, n_stage - 1))

        @pl.when(k >= N_CHUNK)
        def _():
            for s in range(N_B):
                landed(hres.at[kc, s], s_hres0.at[kc, s])
                landed(hres.at[kc, s], s_hres1.at[kc, s])

        for s in range(N_B):
            landed(rec_m.at[k, s], r_hm.at[k, s])
            landed(hrec1.at[kc, s], s_hsum.at[kc, s])
            hres[kc, s] = (hrec1[kc, s] + rec_m[k, s]).astype(BF16)
            remote(hres.at[kc, s], res_b.at[k, s], s_hres0.at[kc, s], r_b.at[k, s], to_stage, end_of).start()
            remote(hres.at[kc, s], res_b.at[k, s], s_hres1.at[kc, s], r_b.at[k, s], to_stage, line).start()

            @pl.when(jnp.logical_and(k >= N_CHUNK, stage == mirror))
            def _():
                res_b[k, s] = hres[kc, s]
                remote(hres.at[kc, s], res_b.at[k, s], s_hres2.at[kc, s], r_b.at[k, s], stage, end_of).start()

    def help_forward(k):
        kc = lax.rem(k, N_CHUNK)

        @pl.when(k >= N_CHUNK)
        def _():
            for s in range(N_B):
                landed(hrec0.at[kc, s], s_hsum.at[kc, s])

        for s in range(N_B):
            landed(rec_m.at[k, s], r_hm.at[k, s])
            remote(rec_m.at[k, s], hrec0.at[kc, s], s_hsum.at[kc, s], r_h0.at[kc, s], stage, mid_of).start()

    def help_stage(finish_early):
        @pl.when(is_end)
        def _():
            @pl.loop(0, 2 * N_CHUNK)
            def _(k):
                help_forward(k)
                finish_early(k)

        @pl.when(is_mid)
        def _():
            @pl.loop(0, 2 * N_CHUNK)
            def _(k):
                help_first(k)

                @pl.when(k == N_CHUNK + 1)
                def _():
                    help_second(k - 1)

                @pl.when(k != N_CHUNK)
                def _():
                    help_second(k)

                finish_early(k)

    def relay(k):
        @pl.when(is_mid)
        def _():
            @pl.when(jnp.logical_and(k >= 1, k <= 2 * N_CHUNK))
            def _():
                sum_first(k - 1)

            @pl.when(jnp.logical_and(k >= 2, k <= 2 * N_CHUNK + 1))
            def _():
                sum_second(k - 2)

    def add_sum(c, k, remote_a, remote_b=None):
        @pl.when(remote_a)
        def _():
            for s in range(N_A):
                landed(res_a.at[k, s], r_a.at[k, s])

        for s in range(N_A):
            at = pl.ds(s * sub, sub)
            hb[c, :, at] = (hb[c, :, at].astype(F32) + res_a[k, s].astype(F32)).astype(BF16)
        for s in range(N_B):
            at = pl.ds((N_A + s) * sub, sub)
            if remote_b is None:
                landed(res_b.at[k, s], r_b.at[k, s])
            else:
                @pl.when(remote_b)
                def _():
                    landed(res_b.at[k, s], r_b.at[k, s])
            hb[c, :, at] = (hb[c, :, at].astype(F32) + res_b[k, s].astype(F32)).astype(BF16)

    def partials(k, act, weight, depth):
        kc = lax.rem(k, N_CHUNK)
        for b_half in (True, False):
            base, count = (N_A, N_B) if b_half else (0, N_A)
            got = dot(act, weight[pl.ds(0, depth), pl.ds(base * sub, count * sub)])
            for s in range(count):
                part[kc, base + s] = got[:, s * sub:(s + 1) * sub]
            send_part(k, b_half)

    def attention(c):
        slot = lax.rem(c, 2)
        landed(hb.at[c], r_h.at[c])

        @pl.when(stage > 0)
        def _():
            add_sum(c, N_CHUNK + c, stage > 0)

        @pl.when(c == 0)
        def _():
            for one in loads[:3]:
                one.wait()

        normed = norm_rows(hb[c], gain_a[...])
        base = pl.multiple_of(c * rows, rows)
        cosv = cos_t[pl.ds(base, rows), :]
        sinv = sin_t[pl.ds(base, rows), :]

        def rope(vals):
            vals32 = vals.astype(BF16).astype(F32)
            return (vals32 * cosv + pltpu.roll(vals32, head_dim // 2, 1) * sinv).astype(BF16)

        nb[...] = normed
        got_k = dot(nb[...], wk[...])
        got_v = dot(nb[...], wv[...])
        for g in range(kv_heads):
            at = pl.ds(g * head_dim, head_dim)
            rotated = rope(got_k[:, g * head_dim:(g + 1) * head_dim])
            kn[c, :, at] = rotated
            mix[0, pl.ds(g, rows, stride=kv_heads), :] = rotated.astype(F32)
            mix[1, pl.ds(g, rows, stride=kv_heads), :] = got_v[:, g * head_dim:(g + 1) * head_dim]
        vn[c] = got_v.astype(BF16)
        ko[c] = mix[0].astype(BF16)
        vo[c] = mix[1].astype(BF16)
        pltpu.make_async_copy(ko.at[c], k_out.at[c], s_rows.at[0, c]).start()
        pltpu.make_async_copy(vo.at[c], v_out.at[c], s_rows.at[1, c]).start()
        got_q = dot(nb[...], wq[...])
        for h in range(n_head):
            qb[:, pl.ds(h * head_dim, head_dim)] = rope(got_q[:, h * head_dim:(h + 1) * head_dim])

        for one in load_kv(c, slot):
            one.wait()
        scale = head_dim ** -0.5
        keys = slots.shape[1]
        n_quad = GROUP // quad
        rows_id = lax.broadcasted_iota(jnp.int32, (GROUP * n_head, keys), 0)
        quad_of = lax.rem(rows_id, GROUP) // quad
        slot_of = slots[...]
        groups = range(rows // GROUP)
        queries = []
        scores = []
        for g in groups:
            rows_at = pl.ds(g * GROUP, GROUP)
            queries.append(jnp.concatenate([qb[rows_at, pl.ds(h * head_dim, head_dim)] for h in range(n_head)], axis=0))
            picked = None
            for j in range(n_quad):
                key_block = kb[slot, pl.ds(g * GROUP * keys_per_row + j * keys, keys), :]
                one = lax.dot_general(queries[g], key_block, (((1,), (1,)), ((), ())), preferred_element_type=F32)
                picked = one if picked is None else jnp.where(quad_of == j, one, picked)
            scores.append(picked * scale)
        probs = []
        probs_new = []
        values_new = []
        for g in groups:
            rows_at = pl.ds(g * GROUP, GROUP)
            key_new = jnp.concatenate([kn[c, rows_at, pl.ds((h // per_kv) * head_dim, head_dim)] for h in range(n_head)], axis=0)
            values_new.append(jnp.concatenate([vn[c, rows_at, pl.ds((h // per_kv) * head_dim, head_dim)] for h in range(n_head)], axis=0))
            score_new = jnp.sum(queries[g].astype(F32) * key_new.astype(F32), axis=-1, keepdims=True) * scale
            p_rows = pos[pl.ds(pl.multiple_of(base + g * GROUP, GROUP), GROUP), :]
            p_wide = jnp.concatenate([jnp.concatenate([p_rows] * (keys // p_rows.shape[1]), axis=1)] * n_head, axis=0)
            valid = slot_of < p_wide
            masked = jnp.where(valid, scores[g], -jnp.inf)
            top = jnp.maximum(jnp.max(masked, axis=-1, keepdims=True), score_new)
            exps = jnp.exp(masked - top)
            exp_new = jnp.exp(score_new - top)
            total = jnp.sum(exps, axis=-1, keepdims=True) + exp_new
            probs.append(exps / total)
            probs_new.append((exp_new / total).astype(BF16).astype(F32))
        for g in groups:
            context = None
            for j in range(n_quad):
                val_block = vb[slot, pl.ds(g * GROUP * keys_per_row + j * keys, keys), :]
                one = dot(jnp.where(quad_of == j, probs[g], 0.0).astype(BF16), val_block)
                context = one if context is None else context + one
            context = (context + probs_new[g] * values_new[g].astype(F32)).astype(BF16)
            for h in range(n_head):
                cb[pl.ds(g * GROUP, GROUP), pl.ds(h * head_dim, head_dim)] = context[h * GROUP:(h + 1) * GROUP]

    def attn_part(c):
        @pl.when(c + 1 < N_CHUNK)
        def _():
            for one in load_kv(c + 1, lax.rem(c + 1, 2)):
                one.start()

        attention(c)

        @pl.when(c == 0)
        def _():
            loads[3].wait()

            @pl.when(stage == 0)
            def _():
                for one in loads[4:7]:
                    one.start()
                pl.semaphore_wait(barrier, n_stage * n_tp)

        partials(c, cb[...], wd, o_rows)

        @pl.when(c == N_CHUNK - 1)
        def _():
            loads[7].start()

    def mlp_part(k):
        c = k - N_CHUNK
        add_sum(c, c, is_end)
        nb[...] = norm_rows(hb[c], gain_m[...])

        @pl.when(c == 0)
        def _():
            for one in loads[4:6]:
                one.wait()

        for at, size in column_blocks(wg.shape[1], 512):
            gate = dot(nb[...], wg[:, pl.ds(at, size)]).astype(BF16).astype(F32)
            up = dot(nb[...], wu[:, pl.ds(at, size)]).astype(BF16).astype(F32)
            ab[:, pl.ds(at, size)] = (gate * jax.nn.sigmoid(gate) * up).astype(BF16)

        @pl.when(c == 0)
        def _():
            for one in loads[6:]:
                one.wait()

        wait_part_sends(k - N_CHUNK)
        partials(k, ab[...], wd, wd.shape[0])

        remote(hb.at[c], hb.at[c], s_h.at[c], r_h.at[c], after, line).start()

    def finish(c, at_last):
        if at_last:
            landed(hb.at[c], s_h.at[c])
            add_sum(c, N_CHUNK + c, is_end)
        else:
            landed(hb.at[c], r_h.at[c])
            add_sum(c, N_CHUNK + c, stage == mirror, is_end)
        hb[c] = norm_rows(hb[c], gain_f[...].reshape(1, hb.shape[2]))
        remote(hb.at[c], out.at[c], s_fwd.at[c], r_out.at[c], stage - 1, line).start()
        pltpu.make_async_copy(hb.at[c], out.at[c], s_out.at[c]).start()

    def finish_mirror(k):
        @pl.when(jnp.logical_and(stage == mirror, k > N_CHUNK))
        def _():
            finish(k - N_CHUNK - 1, False)

    def compute_stage():
        @pl.loop(0, N_CHUNK)
        def _(k):
            attn_part(k)
            relay(k)

        @pl.loop(N_CHUNK, 2 * N_CHUNK)
        def _(k):
            mlp_part(k)
            relay(k)

        @pl.loop(2 * N_CHUNK, 3 * N_CHUNK)
        def _(k):
            @pl.when(stage == last)
            def _():
                finish(k - 2 * N_CHUNK, True)

            relay(k)

    def drain_compute():
        @pl.loop(0, N_CHUNK)
        def _(c):
            wait_part_sends(c)
            for i, (ref, dst) in enumerate(((ko, k_out), (vo, v_out))):
                landed(ref.at[c], s_rows.at[i, c])

            @pl.when(stage < last)
            def _():
                landed(hb.at[c], s_h.at[c])

            @pl.when(is_mid)
            def _():
                for s in range(N_A):
                    landed(res_a.at[c, s], s_res.at[c, s])
                    landed(res_a.at[c, s], s_res2.at[c, s])

                @pl.when(stage == last)
                def _():
                    for s in range(N_A):
                        landed(res_a.at[c, s], s_res3.at[c, s])

    @pl.when(side == 1)
    def _():
        help_stage(lambda k: None)

    compute_stage()
    drain_compute()

    @pl.when(side == 0)
    def _():
        help_stage(finish_mirror)

        @pl.when(stage == mirror)
        def _():
            finish(N_CHUNK - 1, False)

    @pl.loop(0, N_CHUNK)
    def _(c):
        @pl.when(is_mid)
        def _():
            for s in range(N_B):
                landed(hres.at[c, s], s_hres0.at[c, s])
                landed(hres.at[c, s], s_hres1.at[c, s])

            @pl.when(stage == mirror)
            def _():
                for s in range(N_B):
                    landed(hres.at[c, s], s_hres2.at[c, s])

        @pl.when(is_end)
        def _():
            for s in range(N_B):
                landed(hrec0.at[c, s], s_hsum.at[c, s])

        spreads = jnp.logical_or(stage == last, stage == mirror)

        @pl.when(spreads)
        def _():
            landed(hb.at[c], s_out.at[c])
            landed(hb.at[c], s_fwd.at[c])

        @pl.when(jnp.logical_not(spreads))
        def _():
            landed(out.at[c], r_out.at[c])


def copy_kernel(*refs):
    count = len(refs) // 4
    sources, results, staged, sems = (refs[i * count:(i + 1) * count] for i in range(4))
    n = N_CHUNK
    into = [[pltpu.make_async_copy(a.at[c], v.at[c], m.at[0, c]) for c in range(n)] for a, v, m in zip(sources, staged, sems)]
    back = [[pltpu.make_async_copy(v.at[c], o.at[c], m.at[1, c]) for c in range(n)] for o, v, m in zip(results, staged, sems)]
    for c in range(n):
        for one in into:
            one[c].start()
    for c in range(n):
        for one, two in zip(into, back):
            one[c].wait()
            two[c].start()
    for c in range(n):
        for two in back:
            two[c].wait()


def copied(arrays):
    anywhere = pl.BlockSpec(memory_space=pl.ANY)
    return pl.pallas_call(
        copy_kernel,
        out_shape=[jax.ShapeDtypeStruct(a.shape, a.dtype) for a in arrays],
        in_specs=[anywhere] * len(arrays),
        out_specs=[anywhere] * len(arrays),
        scratch_shapes=[pltpu.VMEM(a.shape, a.dtype) for a in arrays] + [pltpu.SemaphoreType.DMA((2, N_CHUNK)) for _ in arrays],
    )(*arrays)


def solution(mesh):
    n_stage = mesh.shape['pp']
    n_tp = mesh.shape['tp']
    cache_spec = P('pp', 'dp', None, 'tp', None)
    gain_spec = P('pp', None)
    col_spec = P('pp', None, 'tp')
    row_spec = P('pp', 'tp', None)
    rows_spec = P('pp', 'dp', 'tp', None)

    def stage_fn(hidden_in, positions, k_cache, v_cache, attn_gain, w_q, w_k, w_v, w_o, mlp_gain, w_gate, w_up, w_down, final_gain):
        batch, d_model = hidden_in.shape
        _, _, cache_len, kv_local, head_dim = k_cache.shape
        rows = batch // N_CHUNK
        d_attn = w_q.shape[2]
        kv_width = kv_local * head_dim
        d_ff = w_gate.shape[2]
        sub = d_model // (N_A + N_B)
        n_head = d_attn // head_dim
        keys = rows * cache_len * kv_local
        score_keys = 4 * cache_len * kv_local
        inverse = ROPE_THETA ** (-np.arange(0, head_dim, 2).astype(np.float32) / head_dim)
        inv_freq = jnp.asarray(np.concatenate([inverse, inverse])[None].astype(np.float32))
        anywhere = pl.BlockSpec(memory_space=pl.ANY)
        vmem = pl.BlockSpec(memory_space=pltpu.VMEM)
        dma = pltpu.SemaphoreType.DMA
        a_blocks = (N_CHUNK, N_A)
        b_blocks = (N_CHUNK, N_B)
        tile = (rows, sub)
        call = pl.pallas_call(
            functools.partial(step_kernel, n_stage, n_tp),
            out_shape=[
                jax.ShapeDtypeStruct((N_CHUNK, rows, d_model), BF16),
                jax.ShapeDtypeStruct((N_CHUNK, rows * kv_local, head_dim), BF16),
                jax.ShapeDtypeStruct((N_CHUNK, rows * kv_local, head_dim), BF16),
            ],
            in_specs=[anywhere, vmem, vmem, anywhere, anywhere, vmem] + [anywhere] * 4 + [vmem] + [anywhere] * 3 + [vmem],
            out_specs=[anywhere] * 3,
            scratch_shapes=[
                pltpu.VMEM((d_model, d_attn), BF16),
                pltpu.VMEM((d_model, kv_width), BF16),
                pltpu.VMEM((d_model, kv_width), BF16),
                pltpu.VMEM((d_model, d_ff), BF16),
                pltpu.VMEM((d_model, d_ff), BF16),
                pltpu.VMEM((d_ff, d_model), BF16),
                pltpu.VMEM((2, keys, head_dim), BF16),
                pltpu.VMEM((2, keys, head_dim), BF16),
                pltpu.VMEM((N_CHUNK, rows, d_model), BF16),
                pltpu.VMEM((rows, d_model), BF16),
                pltpu.VMEM((rows, d_attn), BF16),
                pltpu.VMEM((N_CHUNK, rows, kv_width), BF16),
                pltpu.VMEM((N_CHUNK, rows, kv_width), BF16),
                pltpu.VMEM((N_CHUNK, rows * kv_local, head_dim), BF16),
                pltpu.VMEM((N_CHUNK, rows * kv_local, head_dim), BF16),
                pltpu.VMEM((2, rows * kv_local, head_dim), F32),
                pltpu.VMEM((rows, d_attn), BF16),
                pltpu.VMEM((rows, d_ff), BF16),
                pltpu.VMEM((GROUP * n_head, score_keys), jnp.int32),
                pltpu.VMEM((batch, 128), jnp.int32),
                pltpu.VMEM((batch, head_dim), F32),
                pltpu.VMEM((batch, head_dim), F32),
                pltpu.VMEM((N_CHUNK, N_A + N_B) + tile, F32),
                pltpu.VMEM(a_blocks + tile, F32),
                pltpu.VMEM((2 * N_CHUNK, max(N_A, N_B)) + tile, F32),
                pltpu.VMEM((2 * N_CHUNK, N_A) + tile, BF16),
                pltpu.VMEM((2 * N_CHUNK, N_B) + tile, BF16),
                pltpu.VMEM(b_blocks + tile, F32),
                pltpu.VMEM(b_blocks + tile, F32),
                pltpu.VMEM(b_blocks + tile, BF16),
                dma((8,)), dma((2, 2)), dma((2, N_CHUNK)), dma((N_CHUNK,)), dma((N_CHUNK,)),
                dma((N_CHUNK,)), dma((N_CHUNK,)), dma((N_CHUNK,)),
                dma((N_CHUNK, N_A + N_B)), dma(a_blocks), dma(a_blocks), dma(a_blocks), dma(a_blocks),
                dma(a_blocks), dma((2 * N_CHUNK, N_A)), dma((2 * N_CHUNK, N_A)), dma((2 * N_CHUNK, N_B)),
                dma(b_blocks), dma(b_blocks), dma(b_blocks), dma(b_blocks), dma(b_blocks), dma(b_blocks), dma((2 * N_CHUNK, N_B)),
            ],
            compiler_params=pltpu.CompilerParams(collective_id=0, has_side_effects=True, vmem_limit_bytes=67043328),
        )
        out, k_rows, v_rows = copied(call(
            hidden_in.reshape(N_CHUNK, rows, d_model), positions.reshape(-1, 128), inv_freq,
            k_cache.reshape(N_CHUNK, keys, head_dim), v_cache.reshape(N_CHUNK, keys, head_dim),
            attn_gain, w_q[0], w_k[0], w_v[0], w_o[0], mlp_gain, w_gate[0], w_up[0], w_down[0], final_gain))
        shape = (1, batch, kv_local, head_dim)
        return out.reshape(batch, d_model), k_rows.reshape(shape), v_rows.reshape(shape)

    return jax.shard_map(
        stage_fn,
        mesh=mesh,
        in_specs=(P('dp', None), P('dp'), cache_spec, cache_spec, gain_spec, col_spec, col_spec, col_spec, row_spec, gain_spec, col_spec, col_spec, row_spec, P(None)),
        out_specs=(P('dp', None), rows_spec, rows_spec),
        check_vma=False,
    )
```

```python
import functools

import jax
import jax.numpy as jnp
import numpy as np
from jax import lax
from jax.experimental import pallas as pl
from jax.experimental.pallas import tpu as pltpu
from jax.sharding import PartitionSpec as P

RMS_EPS = 1e-5
ROPE_THETA = 500000.0
BF16 = jnp.bfloat16
F32 = jnp.float32
MESH = pl.DeviceIdType.MESH

N_CHUNK = 4
N_A = 6
N_B = 4
GROUP = 16


def norm_rows(rows, gain):
    rows32 = rows.astype(F32)
    mean_sq = jnp.mean(rows32 * rows32, axis=-1, keepdims=True)
    return (rows32 * lax.rsqrt(mean_sq + RMS_EPS) * gain.astype(F32)).astype(BF16)


def dot(a, b):
    return jnp.dot(a, b, preferred_element_type=F32)


def column_blocks(width, size):
    return [(at, min(size, width - at)) for at in range(0, width, size)]


def step_kernel(
    n_stage, n_tp,
    hid, pos_row, inv_freq, k_hbm, v_hbm, gain_a, w_q, w_k, w_v, w_o, gain_m, w_g, w_u, w_d, gain_f,
    out, k_out, v_out,
    wq, wk, wv, wg, wu, wd, kb, vb, hb, nb, qb, kn, vn, ko, vo, mix, cb, ab, slots, pos, cos_t, sin_t,
    part, rec_e, rec_m, res_a, res_b, hrec0, hrec1, hres,
    s_w, s_kv, s_rows, s_out, s_fwd,
    r_h, s_h, r_out, s_part, s_sum, s_res, s_res2, s_res3, r_e, r_m, r_a, r_b,
    s_hsum, s_hres0, s_hres1, s_hres2, r_h0, r_h1, r_hm,
):
    rows = hb.shape[1]
    sub = part.shape[3]
    d_attn = cb.shape[1]
    kv_width = kn.shape[2]
    head_dim = kb.shape[2]
    n_head = d_attn // head_dim
    kv_heads = kv_width // head_dim
    per_kv = n_head // kv_heads
    cache_len = kb.shape[1] // (rows * kv_heads)
    stage = lax.axis_index('pp')
    line = lax.axis_index('tp')
    side = stage // 2
    helped = lax.rem(stage + 2, n_stage)
    is_mid = jnp.logical_or(line == 1, line == n_tp - 2)
    is_end = jnp.logical_not(is_mid)
    mid_of = jnp.where(line < n_tp // 2, 1, n_tp - 2)
    end_of = jnp.where(line < n_tp // 2, 0, n_tp - 1)
    other_mid = n_tp - 1 - line
    last = n_stage - 1
    mirror = last - 2
    after = jnp.where(stage < last, stage + 1, mirror)

    def remote(src, dst, send, recv, to_stage, to_line):
        return pltpu.make_async_remote_copy(
            src_ref=src, dst_ref=dst, send_sem=send, recv_sem=recv,
            device_id={'pp': to_stage, 'tp': to_line}, device_id_type=MESH)

    def stream(c):
        return hb.at[c, :, pl.ds(N_A * sub, N_B * sub)]

    def landed(ref, sem):
        pltpu.make_async_copy(ref, ref, sem).wait()

    barrier = pltpu.get_barrier_semaphore()
    for other_stage in range(n_stage):
        for other_line in range(n_tp):
            pl.semaphore_signal(barrier, inc=1, device_id={'pp': other_stage, 'tp': other_line}, device_id_type=MESH)

    @pl.when(stage == 0)
    def _():
        for c in range(N_CHUNK):
            pltpu.make_async_copy(hid.at[c], hb.at[c], r_h.at[c]).start()

    def load_kv(c, slot):
        return (pltpu.make_async_copy(k_hbm.at[c], kb.at[slot], s_kv.at[0, slot]),
                pltpu.make_async_copy(v_hbm.at[c], vb.at[slot], s_kv.at[1, slot]))

    o_rows = w_o.shape[0]
    loads = [
        pltpu.make_async_copy(w_q, wq, s_w.at[0]),
        pltpu.make_async_copy(w_k, wk, s_w.at[1]),
        pltpu.make_async_copy(w_v, wv, s_w.at[2]),
        pltpu.make_async_copy(w_o, wd.at[pl.ds(0, o_rows)], s_w.at[3]),
        pltpu.make_async_copy(w_g, wg, s_w.at[4]),
        pltpu.make_async_copy(w_u, wu, s_w.at[5]),
        pltpu.make_async_copy(w_d.at[pl.ds(o_rows, w_d.shape[0] - o_rows)], wd.at[pl.ds(o_rows, w_d.shape[0] - o_rows)], s_w.at[6]),
        pltpu.make_async_copy(w_d.at[pl.ds(0, o_rows)], wd.at[pl.ds(0, o_rows)], s_w.at[7]),
    ]
    for one in loads[1:3] + loads[:1]:
        one.start()
    for one in load_kv(0, 0):
        one.start()
    loads[3].start()

    @pl.when(stage > 0)
    def _():
        for one in loads[4:7]:
            one.start()
        pl.semaphore_wait(barrier, n_stage * n_tp)

    row_id = lax.broadcasted_iota(jnp.int32, slots.shape, 0)
    col_id = lax.broadcasted_iota(jnp.int32, slots.shape, 1)
    keys_per_row = cache_len * kv_heads
    quad = slots.shape[1] // keys_per_row
    same_row = lax.rem(row_id, quad) == col_id // keys_per_row
    same_head = lax.rem(col_id, kv_heads) == row_id // (GROUP * per_kv)
    slots[...] = jnp.where(jnp.logical_and(same_row, same_head), lax.rem(col_id, keys_per_row) // kv_heads, cache_len)

    square = (128, 128)
    on_diag = lax.broadcasted_iota(jnp.int32, square, 0) == lax.broadcasted_iota(jnp.int32, square, 1)
    first_half = lax.broadcasted_iota(jnp.int32, square, 1) < head_dim // 2
    for b in range(pos_row.shape[0]):
        wide = jnp.where(on_diag, jnp.broadcast_to(pos_row[pl.ds(b, 1), :], square), 0).astype(F32)
        column = jnp.broadcast_to(jnp.sum(wide, axis=1, keepdims=True), square)
        at = pl.ds(b * 128, 128)
        pos[at, :] = column.astype(jnp.int32)
        angles = column * inv_freq[...]
        cos_t[at, :] = jnp.cos(angles)
        sines = jnp.sin(angles)
        sin_t[at, :] = jnp.where(first_half, -sines, sines)

    def send_part(k, b_half):
        kc = lax.rem(k, N_CHUNK)
        if b_half:
            @pl.when(is_end)
            def _():
                for s in range(N_B):
                    remote(part.at[kc, N_A + s], rec_m.at[k, s], s_part.at[kc], r_hm.at[k, s], helped, line).start()

            @pl.when(is_mid)
            def _():
                for s in range(N_B):
                    remote(part.at[kc, N_A + s], hrec1.at[kc, s], s_part.at[kc], r_h1.at[kc, s], helped, line).start()
        else:
            @pl.when(is_end)
            def _():
                for s in range(N_A):
                    remote(part.at[kc, s], rec_e.at[kc, s], s_part.at[kc], r_e.at[kc, s], stage, mid_of).start()

    def wait_part_sends(k):
        kc = lax.rem(k, N_CHUNK)
        @pl.when(is_end)
        def _():
            landed(part.at[kc], s_part.at[kc])

        @pl.when(is_mid)
        def _():
            landed(part.at[kc, pl.ds(N_A, N_B)], s_part.at[kc])
            landed(part.at[kc, pl.ds(0, N_A)], s_sum.at[kc])

    def sum_first(k):
        kc = lax.rem(k, N_CHUNK)
        for s in range(N_A):
            landed(rec_e.at[kc, s], r_e.at[kc, s])
            part[kc, s] = part[kc, s] + rec_e[kc, s]
            remote(part.at[kc, s], rec_m.at[k, s], s_sum.at[kc], r_m.at[k, s], stage, other_mid).start()

    def sum_second(k):
        kc = lax.rem(k, N_CHUNK)
        to_stage = jnp.where(k < N_CHUNK, stage, jnp.minimum(stage + 1, n_stage - 1))

        @pl.when(k >= N_CHUNK)
        def _():
            landed(res_a.at[kc], s_res.at[kc])

        for s in range(N_A):
            landed(rec_m.at[k, s], r_m.at[k, s])
            summed = (part[kc, s] + rec_m[k, s]).astype(BF16)
            carried = hb[kc, :, pl.ds(s * sub, sub)]
            res_a[k, s] = jnp.where(k < N_CHUNK, summed, (carried.astype(F32) + summed.astype(F32)).astype(BF16))
            remote(res_a.at[k, s], res_a.at[k, s], s_res.at[kc], r_a.at[k], to_stage, end_of).start()

            @pl.when(k >= N_CHUNK)
            def _():
                remote(res_a.at[k, s], res_a.at[k, s], s_res2.at[kc], r_a.at[k], after, line).start()

            @pl.when(jnp.logical_and(k >= N_CHUNK, stage == last))
            def _():
                remote(res_a.at[k, s], res_a.at[k, s], s_res3.at[kc], r_a.at[k], after, end_of).start()

    def help_first(k):
        kc = lax.rem(k, N_CHUNK)
        for s in range(N_B):
            landed(hrec0.at[kc, s], r_h0.at[kc, s])
            landed(hrec1.at[kc, s], r_h1.at[kc, s])
            hrec1[kc, s] = hrec1[kc, s] + hrec0[kc, s]
            remote(hrec1.at[kc, s], rec_m.at[k, s], s_hsum.at[kc], r_hm.at[k, s], stage, other_mid).start()

    def help_second(k):
        kc = lax.rem(k, N_CHUNK)
        to_stage = jnp.where(k < N_CHUNK, helped, jnp.minimum(helped + 1, n_stage - 1))

        @pl.when(k >= N_CHUNK)
        def _():
            landed(hres.at[kc], s_hres0.at[kc])
            landed(hres.at[kc], s_hres1.at[kc])

        for s in range(N_B):
            landed(rec_m.at[k, s], r_hm.at[k, s])
            if s == 0:
                landed(hrec1.at[kc], s_hsum.at[kc])
            hres[kc, s] = (hrec1[kc, s] + rec_m[k, s]).astype(BF16)
            remote(hres.at[kc, s], res_b.at[k, s], s_hres0.at[kc], r_b.at[k], to_stage, end_of).start()
            remote(hres.at[kc, s], res_b.at[k, s], s_hres1.at[kc], r_b.at[k], to_stage, line).start()

            @pl.when(jnp.logical_and(k >= N_CHUNK, stage == mirror))
            def _():
                res_b[k, s] = hres[kc, s]
                remote(hres.at[kc, s], res_b.at[k, s], s_hres2.at[kc], r_b.at[k], stage, end_of).start()

    def help_forward(k):
        kc = lax.rem(k, N_CHUNK)

        @pl.when(k >= N_CHUNK)
        def _():
            landed(hrec0.at[kc], s_hsum.at[kc])

        for s in range(N_B):
            landed(rec_m.at[k, s], r_hm.at[k, s])
            remote(rec_m.at[k, s], hrec0.at[kc, s], s_hsum.at[kc], r_h0.at[kc, s], stage, mid_of).start()

    def help_stage(finish_early):
        @pl.when(is_end)
        def _():
            @pl.loop(0, 2 * N_CHUNK)
            def _(k):
                help_forward(k)
                finish_early(k)

        @pl.when(is_mid)
        def _():
            @pl.loop(0, 2 * N_CHUNK)
            def _(k):
                help_first(k)

                @pl.when(k == N_CHUNK + 1)
                def _():
                    help_second(k - 1)

                @pl.when(k != N_CHUNK)
                def _():
                    help_second(k)

                finish_early(k)

    def relay(k):
        @pl.when(is_mid)
        def _():
            @pl.when(jnp.logical_and(k >= 1, k <= 2 * N_CHUNK))
            def _():
                sum_first(k - 1)

            @pl.when(jnp.logical_and(k >= 2, k <= 2 * N_CHUNK + 1))
            def _():
                sum_second(k - 2)

    def add_sum(c, k, remote_a, remote_b=None, whole_a=True):
        @pl.when(remote_a)
        def _():
            landed(res_a.at[k], r_a.at[k])

        for s in range(N_A):
            at = pl.ds(s * sub, sub)
            if whole_a:
                hb[c, :, at] = res_a[k, s]
            else:
                hb[c, :, at] = (hb[c, :, at].astype(F32) + res_a[k, s].astype(F32)).astype(BF16)
        if remote_b is None:
            landed(res_b.at[k], r_b.at[k])
        else:
            @pl.when(remote_b)
            def _():
                landed(res_b.at[k], r_b.at[k])

        for s in range(N_B):
            at = pl.ds((N_A + s) * sub, sub)
            hb[c, :, at] = (hb[c, :, at].astype(F32) + res_b[k, s].astype(F32)).astype(BF16)

    def partials(k, act, weight, depth):
        kc = lax.rem(k, N_CHUNK)
        for b_half in (False, True):
            base, count = (N_A, N_B) if b_half else (0, N_A)
            got = dot(act, weight[pl.ds(0, depth), pl.ds(base * sub, count * sub)])
            for s in range(count):
                part[kc, base + s] = got[:, s * sub:(s + 1) * sub]
            send_part(k, b_half)

    def attention(c):
        slot = lax.rem(c, 2)
        @pl.when(stage == 0)
        def _():
            landed(hb.at[c], r_h.at[c])

        @pl.when(stage > 0)
        def _():
            landed(stream(c), r_h.at[c])
            add_sum(c, N_CHUNK + c, stage > 0)

        normed = norm_rows(hb[c], gain_a[...])
        base = pl.multiple_of(c * rows, rows)
        cosv = cos_t[pl.ds(base, rows), :]
        sinv = sin_t[pl.ds(base, rows), :]

        def rope(vals):
            vals32 = vals.astype(BF16).astype(F32)
            return (vals32 * cosv + pltpu.roll(vals32, head_dim // 2, 1) * sinv).astype(BF16)

        nb[...] = normed

        @pl.when(c == 0)
        def _():
            for one in loads[1:3]:
                one.wait()

        got_k = dot(nb[...], wk[...])
        got_v = dot(nb[...], wv[...])
        for g in range(kv_heads):
            at = pl.ds(g * head_dim, head_dim)
            rotated = rope(got_k[:, g * head_dim:(g + 1) * head_dim])
            kn[c, :, at] = rotated
            mix[0, pl.ds(g, rows, stride=kv_heads), :] = rotated.astype(F32)
            mix[1, pl.ds(g, rows, stride=kv_heads), :] = got_v[:, g * head_dim:(g + 1) * head_dim]
        vn[c] = got_v.astype(BF16)
        ko[c] = mix[0].astype(BF16)
        vo[c] = mix[1].astype(BF16)
        pltpu.make_async_copy(ko.at[c], k_out.at[c], s_rows.at[0, c]).start()
        pltpu.make_async_copy(vo.at[c], v_out.at[c], s_rows.at[1, c]).start()

        @pl.when(c == 0)
        def _():
            loads[0].wait()

        got_q = dot(nb[...], wq[...])
        for h in range(n_head):
            qb[:, pl.ds(h * head_dim, head_dim)] = rope(got_q[:, h * head_dim:(h + 1) * head_dim])

        for one in load_kv(c, slot):
            one.wait()
        scale = head_dim ** -0.5
        keys = slots.shape[1]
        n_quad = GROUP // quad
        rows_id = lax.broadcasted_iota(jnp.int32, (GROUP * n_head, keys), 0)
        quad_of = lax.rem(rows_id, GROUP) // quad
        slot_of = slots[...]
        groups = range(rows // GROUP)
        queries = []
        scores = []
        for g in groups:
            rows_at = pl.ds(g * GROUP, GROUP)
            queries.append(jnp.concatenate([qb[rows_at, pl.ds(h * head_dim, head_dim)] for h in range(n_head)], axis=0))
            picked = None
            for j in range(n_quad):
                key_block = kb[slot, pl.ds(g * GROUP * keys_per_row + j * keys, keys), :]
                one = lax.dot_general(queries[g], key_block, (((1,), (1,)), ((), ())), preferred_element_type=F32)
                picked = one if picked is None else jnp.where(quad_of == j, one, picked)
            scores.append(picked * scale)
        probs = []
        probs_new = []
        values_new = []
        for g in groups:
            rows_at = pl.ds(g * GROUP, GROUP)
            key_new = jnp.concatenate([kn[c, rows_at, pl.ds((h // per_kv) * head_dim, head_dim)] for h in range(n_head)], axis=0)
            values_new.append(jnp.concatenate([vn[c, rows_at, pl.ds((h // per_kv) * head_dim, head_dim)] for h in range(n_head)], axis=0))
            score_new = jnp.sum(queries[g].astype(F32) * key_new.astype(F32), axis=-1, keepdims=True) * scale
            p_rows = pos[pl.ds(pl.multiple_of(base + g * GROUP, GROUP), GROUP), :]
            p_wide = jnp.concatenate([jnp.concatenate([p_rows] * (keys // p_rows.shape[1]), axis=1)] * n_head, axis=0)
            valid = slot_of < p_wide
            masked = jnp.where(valid, scores[g], -jnp.inf)
            top = jnp.maximum(jnp.max(masked, axis=-1, keepdims=True), score_new)
            exps = jnp.exp(masked - top)
            exp_new = jnp.exp(score_new - top)
            total = jnp.sum(exps, axis=-1, keepdims=True) + exp_new
            probs.append(exps / total)
            probs_new.append((exp_new / total).astype(BF16).astype(F32))
        for g in groups:
            context = None
            for j in range(n_quad):
                val_block = vb[slot, pl.ds(g * GROUP * keys_per_row + j * keys, keys), :]
                one = dot(jnp.where(quad_of == j, probs[g], 0.0).astype(BF16), val_block)
                context = one if context is None else context + one
            context = (context + probs_new[g] * values_new[g].astype(F32)).astype(BF16)
            for h in range(n_head):
                cb[pl.ds(g * GROUP, GROUP), pl.ds(h * head_dim, head_dim)] = context[h * GROUP:(h + 1) * GROUP]

    def attn_part(c):
        @pl.when(c + 1 < N_CHUNK)
        def _():
            for one in load_kv(c + 1, lax.rem(c + 1, 2)):
                one.start()

        attention(c)

        @pl.when(c == 0)
        def _():
            loads[3].wait()

            @pl.when(stage == 0)
            def _():
                for one in loads[4:7]:
                    one.start()
                pl.semaphore_wait(barrier, n_stage * n_tp)

        partials(c, cb[...], wd, o_rows)

        @pl.when(c == N_CHUNK - 1)
        def _():
            loads[7].start()

    def mlp_part(k):
        c = k - N_CHUNK
        add_sum(c, c, is_end, whole_a=False)
        nb[...] = norm_rows(hb[c], gain_m[...])

        @pl.when(c == 0)
        def _():
            for one in loads[4:6]:
                one.wait()

        for at, size in column_blocks(wg.shape[1], 512):
            gate = dot(nb[...], wg[:, pl.ds(at, size)]).astype(BF16).astype(F32)
            up = dot(nb[...], wu[:, pl.ds(at, size)]).astype(BF16).astype(F32)
            ab[:, pl.ds(at, size)] = (gate * jax.nn.sigmoid(gate) * up).astype(BF16)

        @pl.when(c == 0)
        def _():
            for one in loads[6:]:
                one.wait()

        wait_part_sends(k - N_CHUNK)
        partials(k, ab[...], wd, wd.shape[0])

        remote(stream(c), stream(c), s_h.at[c], r_h.at[c], after, line).start()

    def finish(c, at_last):
        if at_last:
            landed(stream(c), s_h.at[c])
            add_sum(c, N_CHUNK + c, is_end)
        else:
            landed(stream(c), r_h.at[c])
            add_sum(c, N_CHUNK + c, stage == mirror, is_end)
        hb[c] = norm_rows(hb[c], gain_f[...].reshape(1, hb.shape[2]))
        remote(hb.at[c], out.at[c], s_fwd.at[c], r_out.at[c], stage - 1, line).start()
        pltpu.make_async_copy(hb.at[c], out.at[c], s_out.at[c]).start()

    def finish_mirror(k):
        @pl.when(jnp.logical_and(stage == mirror, k > N_CHUNK))
        def _():
            finish(k - N_CHUNK - 1, False)

    def compute_stage():
        @pl.loop(0, N_CHUNK)
        def _(k):
            attn_part(k)
            relay(k)

        @pl.loop(N_CHUNK, 2 * N_CHUNK)
        def _(k):
            mlp_part(k)
            relay(k)

        @pl.loop(2 * N_CHUNK, 3 * N_CHUNK)
        def _(k):
            @pl.when(stage == last)
            def _():
                finish(k - 2 * N_CHUNK, True)

            relay(k)

    def drain_compute():
        @pl.loop(0, N_CHUNK)
        def _(c):
            wait_part_sends(c)
            for i, (ref, dst) in enumerate(((ko, k_out), (vo, v_out))):
                landed(ref.at[c], s_rows.at[i, c])

            @pl.when(stage < last)
            def _():
                landed(stream(c), s_h.at[c])

            @pl.when(is_mid)
            def _():
                landed(res_a.at[c], s_res.at[c])
                landed(res_a.at[c], s_res2.at[c])

                @pl.when(stage == last)
                def _():
                    landed(res_a.at[c], s_res3.at[c])

    @pl.when(side == 1)
    def _():
        help_stage(lambda k: None)

    compute_stage()
    drain_compute()

    @pl.when(side == 0)
    def _():
        help_stage(finish_mirror)

        @pl.when(stage == mirror)
        def _():
            finish(N_CHUNK - 1, False)

    @pl.loop(0, N_CHUNK)
    def _(c):
        @pl.when(is_mid)
        def _():
            landed(hres.at[c], s_hres0.at[c])
            landed(hres.at[c], s_hres1.at[c])

            @pl.when(stage == mirror)
            def _():
                landed(hres.at[c], s_hres2.at[c])

        @pl.when(is_end)
        def _():
            landed(hrec0.at[c], s_hsum.at[c])

        spreads = jnp.logical_or(stage == last, stage == mirror)

        @pl.when(spreads)
        def _():
            landed(hb.at[c], s_out.at[c])
            landed(hb.at[c], s_fwd.at[c])

        @pl.when(jnp.logical_not(spreads))
        def _():
            landed(out.at[c], r_out.at[c])


def copy_kernel(*refs):
    count = len(refs) // 4
    sources, results, staged, sems = (refs[i * count:(i + 1) * count] for i in range(4))
    n = N_CHUNK
    into = [[pltpu.make_async_copy(a.at[c], v.at[c], m.at[0, c]) for c in range(n)] for a, v, m in zip(sources, staged, sems)]
    back = [[pltpu.make_async_copy(v.at[c], o.at[c], m.at[1, c]) for c in range(n)] for o, v, m in zip(results, staged, sems)]
    for c in range(n):
        for one in into:
            one[c].start()
    for c in range(n):
        for one, two in zip(into, back):
            one[c].wait()
            two[c].start()
    for c in range(n):
        for two in back:
            two[c].wait()


def copied(arrays):
    anywhere = pl.BlockSpec(memory_space=pl.ANY)
    return pl.pallas_call(
        copy_kernel,
        out_shape=[jax.ShapeDtypeStruct(a.shape, a.dtype) for a in arrays],
        in_specs=[anywhere] * len(arrays),
        out_specs=[anywhere] * len(arrays),
        scratch_shapes=[pltpu.VMEM(a.shape, a.dtype) for a in arrays] + [pltpu.SemaphoreType.DMA((2, N_CHUNK)) for _ in arrays],
    )(*arrays)


def solution(mesh):
    n_stage = mesh.shape['pp']
    n_tp = mesh.shape['tp']
    cache_spec = P('pp', 'dp', None, 'tp', None)
    gain_spec = P('pp', None)
    col_spec = P('pp', None, 'tp')
    row_spec = P('pp', 'tp', None)
    rows_spec = P('pp', 'dp', 'tp', None)

    def stage_fn(hidden_in, positions, k_cache, v_cache, attn_gain, w_q, w_k, w_v, w_o, mlp_gain, w_gate, w_up, w_down, final_gain):
        batch, d_model = hidden_in.shape
        _, _, cache_len, kv_local, head_dim = k_cache.shape
        rows = batch // N_CHUNK
        d_attn = w_q.shape[2]
        kv_width = kv_local * head_dim
        d_ff = w_gate.shape[2]
        sub = d_model // (N_A + N_B)
        n_head = d_attn // head_dim
        keys = rows * cache_len * kv_local
        score_keys = 4 * cache_len * kv_local
        inverse = ROPE_THETA ** (-np.arange(0, head_dim, 2).astype(np.float32) / head_dim)
        inv_freq = jnp.asarray(np.concatenate([inverse, inverse])[None].astype(np.float32))
        anywhere = pl.BlockSpec(memory_space=pl.ANY)
        vmem = pl.BlockSpec(memory_space=pltpu.VMEM)
        dma = pltpu.SemaphoreType.DMA
        a_blocks = (N_CHUNK, N_A)
        b_blocks = (N_CHUNK, N_B)
        tile = (rows, sub)
        call = pl.pallas_call(
            functools.partial(step_kernel, n_stage, n_tp),
            out_shape=[
                jax.ShapeDtypeStruct((N_CHUNK, rows, d_model), BF16),
                jax.ShapeDtypeStruct((N_CHUNK, rows * kv_local, head_dim), BF16),
                jax.ShapeDtypeStruct((N_CHUNK, rows * kv_local, head_dim), BF16),
            ],
            in_specs=[anywhere, vmem, vmem, anywhere, anywhere, vmem] + [anywhere] * 4 + [vmem] + [anywhere] * 3 + [vmem],
            out_specs=[anywhere] * 3,
            scratch_shapes=[
                pltpu.VMEM((d_model, d_attn), BF16),
                pltpu.VMEM((d_model, kv_width), BF16),
                pltpu.VMEM((d_model, kv_width), BF16),
                pltpu.VMEM((d_model, d_ff), BF16),
                pltpu.VMEM((d_model, d_ff), BF16),
                pltpu.VMEM((d_ff, d_model), BF16),
                pltpu.VMEM((2, keys, head_dim), BF16),
                pltpu.VMEM((2, keys, head_dim), BF16),
                pltpu.VMEM((N_CHUNK, rows, d_model), BF16),
                pltpu.VMEM((rows, d_model), BF16),
                pltpu.VMEM((rows, d_attn), BF16),
                pltpu.VMEM((N_CHUNK, rows, kv_width), BF16),
                pltpu.VMEM((N_CHUNK, rows, kv_width), BF16),
                pltpu.VMEM((N_CHUNK, rows * kv_local, head_dim), BF16),
                pltpu.VMEM((N_CHUNK, rows * kv_local, head_dim), BF16),
                pltpu.VMEM((2, rows * kv_local, head_dim), F32),
                pltpu.VMEM((rows, d_attn), BF16),
                pltpu.VMEM((rows, d_ff), BF16),
                pltpu.VMEM((GROUP * n_head, score_keys), jnp.int32),
                pltpu.VMEM((batch, 128), jnp.int32),
                pltpu.VMEM((batch, head_dim), F32),
                pltpu.VMEM((batch, head_dim), F32),
                pltpu.VMEM((N_CHUNK, N_A + N_B) + tile, F32),
                pltpu.VMEM(a_blocks + tile, F32),
                pltpu.VMEM((2 * N_CHUNK, max(N_A, N_B)) + tile, F32),
                pltpu.VMEM((2 * N_CHUNK, N_A) + tile, BF16),
                pltpu.VMEM((2 * N_CHUNK, N_B) + tile, BF16),
                pltpu.VMEM(b_blocks + tile, F32),
                pltpu.VMEM(b_blocks + tile, F32),
                pltpu.VMEM(b_blocks + tile, BF16),
                dma((8,)), dma((2, 2)), dma((2, N_CHUNK)), dma((N_CHUNK,)), dma((N_CHUNK,)),
                dma((N_CHUNK,)), dma((N_CHUNK,)), dma((N_CHUNK,)),
                dma((N_CHUNK,)), dma((N_CHUNK,)), dma((N_CHUNK,)), dma((N_CHUNK,)), dma((N_CHUNK,)),
                dma(a_blocks), dma((2 * N_CHUNK, N_A)), dma((2 * N_CHUNK,)), dma((2 * N_CHUNK,)),
                dma((N_CHUNK,)), dma((N_CHUNK,)), dma((N_CHUNK,)), dma((N_CHUNK,)), dma(b_blocks), dma(b_blocks), dma((2 * N_CHUNK, N_B)),
            ],
            compiler_params=pltpu.CompilerParams(collective_id=0, has_side_effects=True, vmem_limit_bytes=67043328),
        )
        out, k_rows, v_rows = copied(call(
            hidden_in.reshape(N_CHUNK, rows, d_model), positions.reshape(-1, 128), inv_freq,
            k_cache.reshape(N_CHUNK, keys, head_dim), v_cache.reshape(N_CHUNK, keys, head_dim),
            attn_gain, w_q[0], w_k[0], w_v[0], w_o[0], mlp_gain, w_gate[0], w_up[0], w_down[0], final_gain))
        shape = (1, batch, kv_local, head_dim)
        return out.reshape(batch, d_model), k_rows.reshape(shape), v_rows.reshape(shape)

    return jax.shard_map(
        stage_fn,
        mesh=mesh,
        in_specs=(P('dp', None), P('dp'), cache_spec, cache_spec, gain_spec, col_spec, col_spec, col_spec, row_spec, gain_spec, col_spec, col_spec, row_spec, P(None)),
        out_specs=(P('dp', None), rows_spec, rows_spec),
        check_vma=False,
    )
```

```python
import functools

import jax
import jax.numpy as jnp
import numpy as np
from jax import lax
from jax.experimental import pallas as pl
from jax.experimental.pallas import tpu as pltpu
from jax.sharding import PartitionSpec as P

RMS_EPS = 1e-5
ROPE_THETA = 500000.0
BF16 = jnp.bfloat16
F32 = jnp.float32
MESH = pl.DeviceIdType.MESH

N_CHUNK = 4
N_A = 6
N_B = 4
GROUP = 16


def norm_rows(rows, gain):
    rows32 = rows.astype(F32)
    mean_sq = jnp.mean(rows32 * rows32, axis=-1, keepdims=True)
    return (rows32 * lax.rsqrt(mean_sq + RMS_EPS) * gain.astype(F32)).astype(BF16)


def dot(a, b):
    return jnp.dot(a, b, preferred_element_type=F32)


def column_blocks(width, size):
    return [(at, min(size, width - at)) for at in range(0, width, size)]


def step_kernel(
    n_stage, n_tp,
    hid, pos_row, inv_freq, k_hbm, v_hbm, gain_a, w_q, w_k, w_v, w_o, gain_m, w_g, w_u, w_d, gain_f,
    out, k_out, v_out,
    wq, wk, wv, wg, wu, wd, kb, vb, hb, nb, qb, kn, vn, ko, vo, mix, cb, ab, slots, pos, cos_t, sin_t,
    part, rec_e, rec_m, res_a, res_b, hrec0, hrec1, hres,
    s_w, s_kv, s_rows, s_out, s_fwd,
    r_h, s_h, r_out, s_part, s_sum, s_res, s_res2, s_res3, r_e, r_m, r_a, r_b,
    s_hsum, s_hres0, s_hres1, s_hres2, r_h0, r_h1, r_hm,
):
    rows = hb.shape[1]
    sub = part.shape[3]
    d_attn = cb.shape[1]
    kv_width = kn.shape[2]
    head_dim = kb.shape[2]
    n_head = d_attn // head_dim
    kv_heads = kv_width // head_dim
    per_kv = n_head // kv_heads
    cache_len = kb.shape[1] // (rows * kv_heads)
    stage = lax.axis_index('pp')
    line = lax.axis_index('tp')
    side = stage // 2
    helped = lax.rem(stage + 2, n_stage)
    is_mid = jnp.logical_or(line == 1, line == n_tp - 2)
    is_end = jnp.logical_not(is_mid)
    mid_of = jnp.where(line < n_tp // 2, 1, n_tp - 2)
    end_of = jnp.where(line < n_tp // 2, 0, n_tp - 1)
    other_mid = n_tp - 1 - line
    last = n_stage - 1
    mirror = last - 2
    after = jnp.where(stage < last, stage + 1, mirror)

    def remote(src, dst, send, recv, to_stage, to_line):
        return pltpu.make_async_remote_copy(
            src_ref=src, dst_ref=dst, send_sem=send, recv_sem=recv,
            device_id={'pp': to_stage, 'tp': to_line}, device_id_type=MESH)

    def stream(c):
        return hb.at[c, :, pl.ds(N_A * sub, N_B * sub)]

    def landed(ref, sem):
        pltpu.make_async_copy(ref, ref, sem).wait()

    barrier = pltpu.get_barrier_semaphore()
    for other_stage in range(n_stage):
        for other_line in range(n_tp):
            pl.semaphore_signal(barrier, inc=1, device_id={'pp': other_stage, 'tp': other_line}, device_id_type=MESH)

    @pl.when(stage == 0)
    def _():
        for c in range(N_CHUNK):
            pltpu.make_async_copy(hid.at[c], hb.at[c], r_h.at[c]).start()

    def load_kv(c, slot):
        return (pltpu.make_async_copy(k_hbm.at[c], kb.at[slot], s_kv.at[0, slot]),
                pltpu.make_async_copy(v_hbm.at[c], vb.at[slot], s_kv.at[1, slot]))

    o_rows = w_o.shape[0]
    loads = [
        pltpu.make_async_copy(w_q, wq, s_w.at[0]),
        pltpu.make_async_copy(w_k, wk, s_w.at[1]),
        pltpu.make_async_copy(w_v, wv, s_w.at[2]),
        pltpu.make_async_copy(w_o, wd.at[pl.ds(0, o_rows)], s_w.at[3]),
        pltpu.make_async_copy(w_g, wg, s_w.at[4]),
        pltpu.make_async_copy(w_u, wu, s_w.at[5]),
        pltpu.make_async_copy(w_d.at[pl.ds(o_rows, w_d.shape[0] - o_rows)], wd.at[pl.ds(o_rows, w_d.shape[0] - o_rows)], s_w.at[6]),
        pltpu.make_async_copy(w_d.at[pl.ds(0, o_rows)], wd.at[pl.ds(0, o_rows)], s_w.at[7]),
    ]
    for one in loads[1:3] + loads[:1]:
        one.start()
    for one in load_kv(0, 0):
        one.start()
    loads[3].start()

    @pl.when(stage > 0)
    def _():
        for one in loads[4:7]:
            one.start()
        pl.semaphore_wait(barrier, n_stage * n_tp)

    row_id = lax.broadcasted_iota(jnp.int32, slots.shape, 0)
    col_id = lax.broadcasted_iota(jnp.int32, slots.shape, 1)
    keys_per_row = cache_len * kv_heads
    quad = slots.shape[1] // keys_per_row
    same_row = lax.rem(row_id, quad) == col_id // keys_per_row
    same_head = lax.rem(col_id, kv_heads) == row_id // (GROUP * per_kv)
    slots[...] = jnp.where(jnp.logical_and(same_row, same_head), lax.rem(col_id, keys_per_row) // kv_heads, cache_len)

    square = (128, 128)
    on_diag = lax.broadcasted_iota(jnp.int32, square, 0) == lax.broadcasted_iota(jnp.int32, square, 1)
    first_half = lax.broadcasted_iota(jnp.int32, square, 1) < head_dim // 2
    for b in range(pos_row.shape[0]):
        wide = jnp.where(on_diag, jnp.broadcast_to(pos_row[pl.ds(b, 1), :], square), 0).astype(F32)
        column = jnp.broadcast_to(jnp.sum(wide, axis=1, keepdims=True), square)
        at = pl.ds(b * 128, 128)
        pos[at, :] = column.astype(jnp.int32)
        angles = column * inv_freq[...]
        cos_t[at, :] = jnp.cos(angles)
        sines = jnp.sin(angles)
        sin_t[at, :] = jnp.where(first_half, -sines, sines)

    def send_part(k, b_half):
        kc = lax.rem(k, N_CHUNK)
        if b_half:
            @pl.when(is_end)
            def _():
                for s in range(N_B):
                    remote(part.at[kc, N_A + s], rec_m.at[k, s], s_part.at[kc], r_hm.at[k, s], helped, line).start()

            @pl.when(is_mid)
            def _():
                for s in range(N_B):
                    remote(part.at[kc, N_A + s], hrec1.at[kc, s], s_part.at[kc], r_h1.at[kc, s], helped, line).start()
        else:
            @pl.when(is_end)
            def _():
                for s in range(N_A):
                    remote(part.at[kc, s], rec_e.at[kc, s], s_part.at[kc], r_e.at[kc, s], stage, mid_of).start()

    def wait_part_sends(k):
        kc = lax.rem(k, N_CHUNK)
        @pl.when(is_end)
        def _():
            landed(part.at[kc], s_part.at[kc])

        @pl.when(is_mid)
        def _():
            landed(part.at[kc, pl.ds(N_A, N_B)], s_part.at[kc])
            landed(part.at[kc, pl.ds(0, N_A)], s_sum.at[kc])

    def sum_first(k):
        kc = lax.rem(k, N_CHUNK)
        for s in range(N_A):
            landed(rec_e.at[kc, s], r_e.at[kc, s])
            part[kc, s] = part[kc, s] + rec_e[kc, s]
            remote(part.at[kc, s], rec_m.at[k, s], s_sum.at[kc], r_m.at[k, s], stage, other_mid).start()

    def sum_second(k):
        kc = lax.rem(k, N_CHUNK)
        to_stage = jnp.where(k < N_CHUNK, stage, jnp.minimum(stage + 1, n_stage - 1))

        @pl.when(k >= N_CHUNK)
        def _():
            landed(res_a.at[kc], s_res.at[kc])

        for s in range(N_A):
            landed(rec_m.at[k, s], r_m.at[k, s])
            summed = (part[kc, s] + rec_m[k, s]).astype(BF16)
            carried = hb[kc, :, pl.ds(s * sub, sub)]
            res_a[k, s] = jnp.where(k < N_CHUNK, summed, (carried.astype(F32) + summed.astype(F32)).astype(BF16))
            remote(res_a.at[k, s], res_a.at[k, s], s_res.at[kc], r_a.at[k], to_stage, end_of).start()

            @pl.when(k >= N_CHUNK)
            def _():
                remote(res_a.at[k, s], res_a.at[k, s], s_res2.at[kc], r_a.at[k], after, line).start()

            @pl.when(jnp.logical_and(k >= N_CHUNK, stage == last))
            def _():
                remote(res_a.at[k, s], res_a.at[k, s], s_res3.at[kc], r_a.at[k], after, end_of).start()

    def help_first(k):
        kc = lax.rem(k, N_CHUNK)
        for s in range(N_B):
            landed(hrec0.at[kc, s], r_h0.at[kc, s])
            landed(hrec1.at[kc, s], r_h1.at[kc, s])
            hrec1[kc, s] = hrec1[kc, s] + hrec0[kc, s]
            remote(hrec1.at[kc, s], rec_m.at[k, s], s_hsum.at[kc], r_hm.at[k, s], stage, other_mid).start()

    def help_second(k):
        kc = lax.rem(k, N_CHUNK)
        to_stage = jnp.where(k < N_CHUNK, helped, jnp.minimum(helped + 1, n_stage - 1))

        @pl.when(k >= N_CHUNK)
        def _():
            landed(hres.at[kc], s_hres0.at[kc])
            landed(hres.at[kc], s_hres1.at[kc])

        for s in range(N_B):
            landed(rec_m.at[k, s], r_hm.at[k, s])
            if s == 0:
                landed(hrec1.at[kc], s_hsum.at[kc])
            hres[kc, s] = (hrec1[kc, s] + rec_m[k, s]).astype(BF16)
            remote(hres.at[kc, s], res_b.at[k, s], s_hres0.at[kc], r_b.at[k], to_stage, end_of).start()
            remote(hres.at[kc, s], res_b.at[k, s], s_hres1.at[kc], r_b.at[k], to_stage, line).start()

            @pl.when(jnp.logical_and(k >= N_CHUNK, stage == mirror))
            def _():
                res_b[k, s] = hres[kc, s]
                remote(hres.at[kc, s], res_b.at[k, s], s_hres2.at[kc], r_b.at[k], stage, end_of).start()

    def help_forward(k):
        kc = lax.rem(k, N_CHUNK)

        @pl.when(k >= N_CHUNK)
        def _():
            landed(hrec0.at[kc], s_hsum.at[kc])

        for s in range(N_B):
            landed(rec_m.at[k, s], r_hm.at[k, s])
            remote(rec_m.at[k, s], hrec0.at[kc, s], s_hsum.at[kc], r_h0.at[kc, s], stage, mid_of).start()

    def help_stage(finish_early):
        @pl.when(is_end)
        def _():
            @pl.loop(0, 2 * N_CHUNK)
            def _(k):
                help_forward(k)
                finish_early(k)

        @pl.when(is_mid)
        def _():
            @pl.loop(0, 2 * N_CHUNK)
            def _(k):
                help_first(k)

                @pl.when(k == N_CHUNK + 1)
                def _():
                    help_second(k - 1)

                @pl.when(k != N_CHUNK)
                def _():
                    help_second(k)

                finish_early(k)

    def relay(k):
        @pl.when(is_mid)
        def _():
            @pl.when(jnp.logical_and(k >= 1, k <= 2 * N_CHUNK))
            def _():
                sum_first(k - 1)

            @pl.when(jnp.logical_and(k >= 2, k <= 2 * N_CHUNK + 1))
            def _():
                sum_second(k - 2)

    def add_sum(c, k, remote_a, remote_b=None, whole_a=True):
        @pl.when(remote_a)
        def _():
            landed(res_a.at[k], r_a.at[k])

        for s in range(N_A):
            at = pl.ds(s * sub, sub)
            if whole_a:
                hb[c, :, at] = res_a[k, s]
            else:
                hb[c, :, at] = (hb[c, :, at].astype(F32) + res_a[k, s].astype(F32)).astype(BF16)
        if remote_b is None:
            landed(res_b.at[k], r_b.at[k])
        else:
            @pl.when(remote_b)
            def _():
                landed(res_b.at[k], r_b.at[k])

        for s in range(N_B):
            at = pl.ds((N_A + s) * sub, sub)
            hb[c, :, at] = (hb[c, :, at].astype(F32) + res_b[k, s].astype(F32)).astype(BF16)

    def partials(k, act, weight, depth):
        kc = lax.rem(k, N_CHUNK)
        for b_half in (False, True):
            base, count = (N_A, N_B) if b_half else (0, N_A)
            got = dot(act, weight[pl.ds(0, depth), pl.ds(base * sub, count * sub)])
            for s in range(count):
                part[kc, base + s] = got[:, s * sub:(s + 1) * sub]
            send_part(k, b_half)

    def attention(c):
        slot = lax.rem(c, 2)
        @pl.when(stage == 0)
        def _():
            landed(hb.at[c], r_h.at[c])

        @pl.when(stage > 0)
        def _():
            landed(stream(c), r_h.at[c])
            add_sum(c, N_CHUNK + c, stage > 0)

        normed = norm_rows(hb[c], gain_a[...])
        base = pl.multiple_of(c * rows, rows)
        cosv = cos_t[pl.ds(base, rows), :]
        sinv = sin_t[pl.ds(base, rows), :]

        def rope(vals):
            vals32 = vals.astype(BF16).astype(F32)
            return (vals32 * cosv + pltpu.roll(vals32, head_dim // 2, 1) * sinv).astype(BF16)

        nb[...] = normed

        @pl.when(c == 0)
        def _():
            for one in loads[1:3]:
                one.wait()

        got_k = dot(nb[...], wk[...])
        got_v = dot(nb[...], wv[...])
        for g in range(kv_heads):
            at = pl.ds(g * head_dim, head_dim)
            rotated = rope(got_k[:, g * head_dim:(g + 1) * head_dim])
            kn[c, :, at] = rotated
            mix[0, pl.ds(g, rows, stride=kv_heads), :] = rotated.astype(F32)
            mix[1, pl.ds(g, rows, stride=kv_heads), :] = got_v[:, g * head_dim:(g + 1) * head_dim]
        vn[c] = got_v.astype(BF16)
        ko[c] = mix[0].astype(BF16)
        vo[c] = mix[1].astype(BF16)
        pltpu.make_async_copy(ko.at[c], k_out.at[c], s_rows.at[0, c]).start()
        pltpu.make_async_copy(vo.at[c], v_out.at[c], s_rows.at[1, c]).start()

        @pl.when(c == 0)
        def _():
            loads[0].wait()

        got_q = dot(nb[...], wq[...])
        for h in range(n_head):
            qb[:, pl.ds(h * head_dim, head_dim)] = rope(got_q[:, h * head_dim:(h + 1) * head_dim])

        for one in load_kv(c, slot):
            one.wait()
        scale = head_dim ** -0.5
        keys = slots.shape[1]
        n_quad = GROUP // quad
        rows_id = lax.broadcasted_iota(jnp.int32, (GROUP * n_head, keys), 0)
        quad_of = lax.rem(rows_id, GROUP) // quad
        slot_of = slots[...]
        groups = range(rows // GROUP)
        queries = []
        scores = []
        for g in groups:
            rows_at = pl.ds(g * GROUP, GROUP)
            queries.append(jnp.concatenate([qb[rows_at, pl.ds(h * head_dim, head_dim)] for h in range(n_head)], axis=0))
            picked = None
            for j in range(n_quad):
                key_block = kb[slot, pl.ds(g * GROUP * keys_per_row + j * keys, keys), :]
                one = lax.dot_general(queries[g], key_block, (((1,), (1,)), ((), ())), preferred_element_type=F32)
                picked = one if picked is None else jnp.where(quad_of == j, one, picked)
            scores.append(picked * scale)
        probs = []
        probs_new = []
        values_new = []
        for g in groups:
            rows_at = pl.ds(g * GROUP, GROUP)
            key_new = jnp.concatenate([kn[c, rows_at, pl.ds((h // per_kv) * head_dim, head_dim)] for h in range(n_head)], axis=0)
            values_new.append(jnp.concatenate([vn[c, rows_at, pl.ds((h // per_kv) * head_dim, head_dim)] for h in range(n_head)], axis=0))
            score_new = jnp.sum(queries[g].astype(F32) * key_new.astype(F32), axis=-1, keepdims=True) * scale
            p_rows = pos[pl.ds(pl.multiple_of(base + g * GROUP, GROUP), GROUP), :]
            p_wide = jnp.concatenate([jnp.concatenate([p_rows] * (keys // p_rows.shape[1]), axis=1)] * n_head, axis=0)
            valid = slot_of < p_wide
            masked = jnp.where(valid, scores[g], -jnp.inf)
            top = jnp.maximum(jnp.max(masked, axis=-1, keepdims=True), score_new)
            exps = jnp.exp(masked - top)
            exp_new = jnp.exp(score_new - top)
            total = jnp.sum(exps, axis=-1, keepdims=True) + exp_new
            probs.append(exps / total)
            probs_new.append((exp_new / total).astype(BF16).astype(F32))
        for g in groups:
            context = None
            for j in range(n_quad):
                val_block = vb[slot, pl.ds(g * GROUP * keys_per_row + j * keys, keys), :]
                one = dot(jnp.where(quad_of == j, probs[g], 0.0).astype(BF16), val_block)
                context = one if context is None else context + one
            context = (context + probs_new[g] * values_new[g].astype(F32)).astype(BF16)
            for h in range(n_head):
                cb[pl.ds(g * GROUP, GROUP), pl.ds(h * head_dim, head_dim)] = context[h * GROUP:(h + 1) * GROUP]

    def attn_part(c):
        @pl.when(c + 1 < N_CHUNK)
        def _():
            for one in load_kv(c + 1, lax.rem(c + 1, 2)):
                one.start()

        attention(c)

        @pl.when(c == 0)
        def _():
            loads[3].wait()

            @pl.when(stage == 0)
            def _():
                for one in loads[4:7]:
                    one.start()
                pl.semaphore_wait(barrier, n_stage * n_tp)

        partials(c, cb[...], wd, o_rows)

        @pl.when(c == N_CHUNK - 1)
        def _():
            loads[7].start()

    def mlp_part(k):
        c = k - N_CHUNK
        add_sum(c, c, is_end, whole_a=False)
        nb[...] = norm_rows(hb[c], gain_m[...])

        @pl.when(c == 0)
        def _():
            for one in loads[4:6]:
                one.wait()

        for at, size in column_blocks(wg.shape[1], 512):
            gate = dot(nb[...], wg[:, pl.ds(at, size)]).astype(BF16).astype(F32)
            up = dot(nb[...], wu[:, pl.ds(at, size)]).astype(BF16).astype(F32)
            ab[:, pl.ds(at, size)] = (gate * jax.nn.sigmoid(gate) * up).astype(BF16)

        @pl.when(c == 0)
        def _():
            for one in loads[6:]:
                one.wait()

        @pl.when(k >= 2 * N_CHUNK - 2)
        def _():
            relay(k)

        wait_part_sends(k - N_CHUNK)
        partials(k, ab[...], wd, wd.shape[0])

        remote(stream(c), stream(c), s_h.at[c], r_h.at[c], after, line).start()

    def finish(c, at_last):
        if at_last:
            landed(stream(c), s_h.at[c])
            add_sum(c, N_CHUNK + c, is_end)
        else:
            landed(stream(c), r_h.at[c])
            add_sum(c, N_CHUNK + c, stage == mirror, is_end)
        hb[c] = norm_rows(hb[c], gain_f[...].reshape(1, hb.shape[2]))
        remote(hb.at[c], out.at[c], s_fwd.at[c], r_out.at[c], stage - 1, line).start()
        pltpu.make_async_copy(hb.at[c], out.at[c], s_out.at[c]).start()

    def finish_mirror(k):
        @pl.when(jnp.logical_and(stage == mirror, k > N_CHUNK))
        def _():
            finish(k - N_CHUNK - 1, False)

    def compute_stage():
        @pl.loop(0, N_CHUNK)
        def _(k):
            attn_part(k)
            relay(k)

        @pl.loop(N_CHUNK, 2 * N_CHUNK)
        def _(k):
            mlp_part(k)

            @pl.when(k < 2 * N_CHUNK - 2)
            def _():
                relay(k)

        @pl.loop(2 * N_CHUNK, 3 * N_CHUNK)
        def _(k):
            @pl.when(stage == last)
            def _():
                finish(k - 2 * N_CHUNK, True)

            relay(k)

    def drain_compute():
        @pl.loop(0, N_CHUNK)
        def _(c):
            wait_part_sends(c)
            for i, (ref, dst) in enumerate(((ko, k_out), (vo, v_out))):
                landed(ref.at[c], s_rows.at[i, c])

            @pl.when(stage < last)
            def _():
                landed(stream(c), s_h.at[c])

            @pl.when(is_mid)
            def _():
                landed(res_a.at[c], s_res.at[c])
                landed(res_a.at[c], s_res2.at[c])

                @pl.when(stage == last)
                def _():
                    landed(res_a.at[c], s_res3.at[c])

    @pl.when(side == 1)
    def _():
        help_stage(lambda k: None)

    compute_stage()
    drain_compute()

    @pl.when(side == 0)
    def _():
        help_stage(finish_mirror)

        @pl.when(stage == mirror)
        def _():
            finish(N_CHUNK - 1, False)

    @pl.loop(0, N_CHUNK)
    def _(c):
        @pl.when(is_mid)
        def _():
            landed(hres.at[c], s_hres0.at[c])
            landed(hres.at[c], s_hres1.at[c])

            @pl.when(stage == mirror)
            def _():
                landed(hres.at[c], s_hres2.at[c])

        @pl.when(is_end)
        def _():
            landed(hrec0.at[c], s_hsum.at[c])

        spreads = jnp.logical_or(stage == last, stage == mirror)

        @pl.when(spreads)
        def _():
            landed(hb.at[c], s_out.at[c])
            landed(hb.at[c], s_fwd.at[c])

        @pl.when(jnp.logical_not(spreads))
        def _():
            landed(out.at[c], r_out.at[c])


def copy_kernel(*refs):
    count = len(refs) // 4
    sources, results, staged, sems = (refs[i * count:(i + 1) * count] for i in range(4))
    n = N_CHUNK
    into = [[pltpu.make_async_copy(a.at[c], v.at[c], m.at[0, c]) for c in range(n)] for a, v, m in zip(sources, staged, sems)]
    back = [[pltpu.make_async_copy(v.at[c], o.at[c], m.at[1, c]) for c in range(n)] for o, v, m in zip(results, staged, sems)]
    for c in range(n):
        for one in into:
            one[c].start()
    for c in range(n):
        for one, two in zip(into, back):
            one[c].wait()
            two[c].start()
    for c in range(n):
        for two in back:
            two[c].wait()


def copied(arrays):
    anywhere = pl.BlockSpec(memory_space=pl.ANY)
    return pl.pallas_call(
        copy_kernel,
        out_shape=[jax.ShapeDtypeStruct(a.shape, a.dtype) for a in arrays],
        in_specs=[anywhere] * len(arrays),
        out_specs=[anywhere] * len(arrays),
        scratch_shapes=[pltpu.VMEM(a.shape, a.dtype) for a in arrays] + [pltpu.SemaphoreType.DMA((2, N_CHUNK)) for _ in arrays],
    )(*arrays)


def solution(mesh):
    n_stage = mesh.shape['pp']
    n_tp = mesh.shape['tp']
    cache_spec = P('pp', 'dp', None, 'tp', None)
    gain_spec = P('pp', None)
    col_spec = P('pp', None, 'tp')
    row_spec = P('pp', 'tp', None)
    rows_spec = P('pp', 'dp', 'tp', None)

    def stage_fn(hidden_in, positions, k_cache, v_cache, attn_gain, w_q, w_k, w_v, w_o, mlp_gain, w_gate, w_up, w_down, final_gain):
        batch, d_model = hidden_in.shape
        _, _, cache_len, kv_local, head_dim = k_cache.shape
        rows = batch // N_CHUNK
        d_attn = w_q.shape[2]
        kv_width = kv_local * head_dim
        d_ff = w_gate.shape[2]
        sub = d_model // (N_A + N_B)
        n_head = d_attn // head_dim
        keys = rows * cache_len * kv_local
        score_keys = 4 * cache_len * kv_local
        inverse = ROPE_THETA ** (-np.arange(0, head_dim, 2).astype(np.float32) / head_dim)
        inv_freq = jnp.asarray(np.concatenate([inverse, inverse])[None].astype(np.float32))
        anywhere = pl.BlockSpec(memory_space=pl.ANY)
        vmem = pl.BlockSpec(memory_space=pltpu.VMEM)
        dma = pltpu.SemaphoreType.DMA
        a_blocks = (N_CHUNK, N_A)
        b_blocks = (N_CHUNK, N_B)
        tile = (rows, sub)
        call = pl.pallas_call(
            functools.partial(step_kernel, n_stage, n_tp),
            out_shape=[
                jax.ShapeDtypeStruct((N_CHUNK, rows, d_model), BF16),
                jax.ShapeDtypeStruct((N_CHUNK, rows * kv_local, head_dim), BF16),
                jax.ShapeDtypeStruct((N_CHUNK, rows * kv_local, head_dim), BF16),
            ],
            in_specs=[anywhere, vmem, vmem, anywhere, anywhere, vmem] + [anywhere] * 4 + [vmem] + [anywhere] * 3 + [vmem],
            out_specs=[anywhere] * 3,
            scratch_shapes=[
                pltpu.VMEM((d_model, d_attn), BF16),
                pltpu.VMEM((d_model, kv_width), BF16),
                pltpu.VMEM((d_model, kv_width), BF16),
                pltpu.VMEM((d_model, d_ff), BF16),
                pltpu.VMEM((d_model, d_ff), BF16),
                pltpu.VMEM((d_ff, d_model), BF16),
                pltpu.VMEM((2, keys, head_dim), BF16),
                pltpu.VMEM((2, keys, head_dim), BF16),
                pltpu.VMEM((N_CHUNK, rows, d_model), BF16),
                pltpu.VMEM((rows, d_model), BF16),
                pltpu.VMEM((rows, d_attn), BF16),
                pltpu.VMEM((N_CHUNK, rows, kv_width), BF16),
                pltpu.VMEM((N_CHUNK, rows, kv_width), BF16),
                pltpu.VMEM((N_CHUNK, rows * kv_local, head_dim), BF16),
                pltpu.VMEM((N_CHUNK, rows * kv_local, head_dim), BF16),
                pltpu.VMEM((2, rows * kv_local, head_dim), F32),
                pltpu.VMEM((rows, d_attn), BF16),
                pltpu.VMEM((rows, d_ff), BF16),
                pltpu.VMEM((GROUP * n_head, score_keys), jnp.int32),
                pltpu.VMEM((batch, 128), jnp.int32),
                pltpu.VMEM((batch, head_dim), F32),
                pltpu.VMEM((batch, head_dim), F32),
                pltpu.VMEM((N_CHUNK, N_A + N_B) + tile, F32),
                pltpu.VMEM(a_blocks + tile, F32),
                pltpu.VMEM((2 * N_CHUNK, max(N_A, N_B)) + tile, F32),
                pltpu.VMEM((2 * N_CHUNK, N_A) + tile, BF16),
                pltpu.VMEM((2 * N_CHUNK, N_B) + tile, BF16),
                pltpu.VMEM(b_blocks + tile, F32),
                pltpu.VMEM(b_blocks + tile, F32),
                pltpu.VMEM(b_blocks + tile, BF16),
                dma((8,)), dma((2, 2)), dma((2, N_CHUNK)), dma((N_CHUNK,)), dma((N_CHUNK,)),
                dma((N_CHUNK,)), dma((N_CHUNK,)), dma((N_CHUNK,)),
                dma((N_CHUNK,)), dma((N_CHUNK,)), dma((N_CHUNK,)), dma((N_CHUNK,)), dma((N_CHUNK,)),
                dma(a_blocks), dma((2 * N_CHUNK, N_A)), dma((2 * N_CHUNK,)), dma((2 * N_CHUNK,)),
                dma((N_CHUNK,)), dma((N_CHUNK,)), dma((N_CHUNK,)), dma((N_CHUNK,)), dma(b_blocks), dma(b_blocks), dma((2 * N_CHUNK, N_B)),
            ],
            compiler_params=pltpu.CompilerParams(collective_id=0, has_side_effects=True, vmem_limit_bytes=67043328),
        )
        out, k_rows, v_rows = copied(call(
            hidden_in.reshape(N_CHUNK, rows, d_model), positions.reshape(-1, 128), inv_freq,
            k_cache.reshape(N_CHUNK, keys, head_dim), v_cache.reshape(N_CHUNK, keys, head_dim),
            attn_gain, w_q[0], w_k[0], w_v[0], w_o[0], mlp_gain, w_gate[0], w_up[0], w_down[0], final_gain))
        shape = (1, batch, kv_local, head_dim)
        return out.reshape(batch, d_model), k_rows.reshape(shape), v_rows.reshape(shape)

    return jax.shard_map(
        stage_fn,
        mesh=mesh,
        in_specs=(P('dp', None), P('dp'), cache_spec, cache_spec, gain_spec, col_spec, col_spec, col_spec, row_spec, gain_spec, col_spec, col_spec, row_spec, P(None)),
        out_specs=(P('dp', None), rows_spec, rows_spec),
        check_vma=False,
    )
```
